256 devices in a mesh: tok: 4 (over y), col: 64 (over z, x, core).
Axes of the slice: x: 4, y: 4, z: 8, core: 2. Of those that a mesh axis runs over, the one named last changes fastest.
Arguments:
- row_bank: bfloat16 [16384, 8192], P(None, 'col'), may hold values from -50 to 50
- token_ids: int32 [6144], P('tok'), may hold values from 0 to 16383
- sign_flips: int32 [8192], P('col'), may hold values from -1 to 1, as said below
- damping: float32 [1], replicated, may hold values from 0.1 to 1
Outputs:
- hessian: float32 [8192, 8192], P('tok', 'col')
The draws below stay inside these ranges and needn't reach their ends.
Inputs may be any that keep to these rules, and one draw needn't show every extreme that they name: `sign_flips`: each entry is -1 or 1.
All inputs are finite; a program needn't handle non-finite values.
Results may differ from the reference program's by a relative error of at most 0.0003.
The reference program's roundings to bfloat16 on the way (of `picked`, `half_turned` and `rotated`) count: a program that leaves them out, or rounds other values in their place, can miss the bound.
Values may be sent and summed in bfloat16 or wider, within the bound.
A program may use at most 128 MiB of HBM per device.

```python
import math
import jax
import jax.numpy as jnp

D = 8192
BLOCK = 32
TOKENS = 6144
BANK = 16384


def draw_sign_flips(key, part):
    return 2 * jax.random.randint(key, (D,), 0, 2, dtype=jnp.int32) - 1


def draw_token_ids(key, part):
    spot = jnp.arange(TOKENS, dtype=jnp.int32)
    start = spot * (BANK // 2) // TOKENS
    jitter = jax.random.randint(jax.random.fold_in(key, 11), (TOKENS,), 0, BANK // 2, dtype=jnp.int32)
    return start + jitter


def draw_row_bank(key, part):
    place = jnp.arange(BANK, dtype=jnp.float32) / BANK
    lift = jax.random.uniform(jax.random.fold_in(key, 21), (BANK,), jnp.float32)
    row_scale = jnp.power(10.0, 0.8 * place + 0.4 * lift)
    col_scale = jnp.exp(jax.random.uniform(jax.random.fold_in(key, 22), (D,), jnp.float32) * math.log(10.0))
    noise = jnp.clip(jax.random.normal(jax.random.fold_in(key, 23), (BANK, D), jnp.float32), -6.0, 6.0)
    values = noise * row_scale[:, None] * col_scale[None, :] / 30.0
    return values.astype(jnp.bfloat16)


def setup_inputs(seed: int = 0) -> dict:
    key_list = jax.random.split(jax.random.key(seed), 5)
    row_bank = draw_row_bank(jax.random.fold_in(key_list[4], 71), 0)
    token_ids = draw_token_ids(jax.random.fold_in(key_list[4], 71), 0)
    sign_flips = draw_sign_flips(jax.random.fold_in(key_list[4], 71), 0)
    damping = jnp.clip(jnp.exp(jax.random.uniform(key_list[3], (1,), jnp.float32, math.log(0.1), math.log(1.0))), 0.1, 1.0)
    return dict(row_bank=row_bank, token_ids=token_ids, sign_flips=sign_flips, damping=damping)


def hadamard(order):
    index_range = jnp.arange(order, dtype=jnp.int32)
    anded = jnp.bitwise_and(index_range[:, None], index_range[None, :])
    parity = jnp.zeros((order, order), jnp.int32)
    for bit_place in range(int(order).bit_length()):
        parity = parity + jnp.bitwise_and(jnp.right_shift(anded, bit_place), 1)
    return (1 - 2 * jnp.bitwise_and(parity, 1)).astype(jnp.float32)

def reference(row_bank, token_ids, sign_flips, damping):
    groups = D // BLOCK
    picked = row_bank[token_ids] * sign_flips.astype(jnp.bfloat16)[None, :]
    grouped_rows = picked.reshape(TOKENS, groups, BLOCK).astype(jnp.float32)
    half_turned = jnp.einsum('rab,bc->rac', grouped_rows, hadamard(BLOCK)).astype(jnp.bfloat16)
    turned = jnp.einsum('rab,ac->rcb', half_turned.astype(jnp.float32), hadamard(groups)) * (1.0 / math.sqrt(D))
    rotated = turned.astype(jnp.bfloat16).reshape(TOKENS, D)
    gram_matrix = jnp.dot(rotated.T, rotated, preferred_element_type=jnp.float32) / TOKENS
    mean_diag = jnp.mean(jnp.diagonal(gram_matrix))
    return gram_matrix + damping[0] * mean_diag * jnp.eye(D, dtype=jnp.float32)
```

```python
import functools
import math

import jax
import jax.numpy as jnp
import numpy as np
from jax import lax
from jax.experimental import pallas as pl
from jax.experimental.pallas import tpu as pltpu
from jax.sharding import Mesh
from jax.sharding import PartitionSpec as P

D = 8192
BLOCK = 32
TOKENS = 6144
COL = ("z", "x", "c")
NY, NZ, NX, NC = 4, 8, 4, 2
TG = TOKENS // (NY * NX)
MESH = pl.DeviceIdType.MESH
NT = (((1,), (1,)), ((), ()))
NN = (((1,), (0,)), ((), ()))


def parity_sign(v):
    v = v ^ (v >> 4)
    v = v ^ (v >> 2)
    v = v ^ (v >> 1)
    return 1 - 2 * (v & 1)


def inner_table():
    r = np.arange(128)
    b_r, a_r = (r >> 4) * 4 + (r & 3), (r >> 2) & 3
    b_c, a_c = r & 31, r >> 5
    bits = np.array([bin(i).count("1") & 1 for i in range(32)])
    signs = 1 - 2 * bits[b_r[:, None] & b_c[None, :]]
    return np.where(a_r[:, None] == a_c[None, :], signs, 0).astype(np.float32)


def outer_table(core, for_rows):
    r = lax.broadcasted_iota(jnp.int32, (512, 1), 0)
    k = lax.broadcasted_iota(jnp.int32, (1, 1024), 1)
    if for_rows:
        c = ((r >> 7) << 6) | ((r & 7) << 3) | ((r >> 5) & 3)
        b_r = (r >> 3) & 3
    else:
        c = ((r >> 6) << 5) | (((r >> 4) & 3) << 3) | ((r >> 2) & 3)
        b_r = r & 3
    c = c | (core << 2)
    a = (((k >> 6) & 7) << 5) | (((k >> 4) & 3) << 3) | ((k >> 9) << 2) | ((k >> 2) & 3)
    sign = parity_sign(c & a)
    return jnp.where(b_r == (k & 3), sign, 0).astype(jnp.float32).astype(jnp.bfloat16)


def column_order():
    o = lax.broadcasted_iota(jnp.int32, (128, 128), 0)
    i = lax.broadcasted_iota(jnp.int32, (128, 128), 1)
    src = (((o >> 2) & 7) << 4) | ((o >> 5) << 2) | (o & 3)
    return (i == src).astype(jnp.float32).astype(jnp.bfloat16)


def kernel(
    picked, hs, out, tr,
    hb, x1, x2, hm, hn, rm, rn, mb, nz, np_, g, ra, rb, ts, trx,
    s1, r1, s2, r2, s3, r3, sn, rn_sem, sm, rm_sem, sy, ry, sr, rr, sl, rl, sd, rd,
    sa, ra_sem, sb, rb_sem, st, rt,
):
    y, z, x, c = (lax.axis_index(n) for n in ("tok", "z", "x", "c"))
    scale = 1.0 / math.sqrt(D)

    def at_x(d):
        return lax.rem(x + d + NX, NX)

    def at_y(d):
        return lax.rem(y + d + NY, NY)

    def at_z(d):
        return lax.rem(z + d + NZ, NZ)

    def copy(src, dst, send, recv, **where):
        return pltpu.make_async_remote_copy(
            src_ref=src, dst_ref=dst, send_sem=send, recv_sem=recv,
            device_id=where, device_id_type=MESH,
        )

    started = []

    def send(*args, **where):
        cp = copy(*args, **where)
        cp.start()
        started.append(cp)

    def arrived(ref, sem):
        copy(ref, ref, sem, sem, c=1 - c).wait_recv()

    barrier = pltpu.get_barrier_semaphore()
    peers = (
        [dict(x=at_x(d)) for d in range(1, NX)]
        + [dict(tok=at_y(d)) for d in range(1, NY)]
        + [dict(z=at_z(d)) for d in range(1, NZ)]
        + [dict(c=1 - c)]
    )
    for where in peers:
        pl.semaphore_signal(barrier, inc=1, device_id=where, device_id_type=MESH)

    for j in range(NX):
        h = lax.dot_general(
            hs[...], picked[j * TG : (j + 1) * TG, :], NT, preferred_element_type=jnp.float32
        )
        hb[j] = h.astype(jnp.bfloat16)
    x1[x] = hb[x]
    pl.semaphore_wait(barrier, len(peers))

    for d in range(1, NX):
        send(hb.at[at_x(d)], x1.at[x], s1.at[d - 1], r1.at[d - 1], x=at_x(d))
    hn[...] = outer_table(c, False)
    for d in range(1, NX):
        arrived(x1.at[at_x(-d)], r1.at[d - 1])

    def piece(zz):
        return x1.at[:, pl.ds(pl.multiple_of(zz * 16, 16), 16), :]

    for d in range(1, NZ):
        send(piece(at_z(d)), x2.at[c, z], s2.at[d - 1], r2.at[d - 1], z=at_z(d))
    send(piece(z), x2.at[c, z], s3.at[0], r3.at[0], c=1 - c)
    x2[c, z] = x1[:, pl.ds(pl.multiple_of(z * 16, 16), 16), :]
    hm[...] = outer_table(c, True)
    for d in range(1, NZ):
        got = x2.at[c, at_z(-d)]
        arrived(got, r2.at[d - 1])
        send(got, got, s3.at[d], r3.at[d], c=1 - c)
    for d in range(NZ):
        arrived(x2.at[1 - c, at_z(-d)], r3.at[d])

    spread = x2[...].reshape(1024, TG)

    def turn(table):
        return (
            lax.dot_general(table[...], spread, NN, preferred_element_type=jnp.float32) * scale
        ).astype(jnp.bfloat16)

    rn[...] = turn(hn).reshape(NZ, 64, TG)
    for d in range(1, NZ):
        send(rn.at[at_z(d)], nz.at[z, y], sn.at[d - 1], rn_sem.at[d - 1], z=at_z(d))
    nz[z, y] = rn[z]
    rows = turn(hm)
    rm[...] = rows.reshape(NY, 128, TG)
    for d in range(1, NY):
        send(rm.at[at_y(d)], mb.at[z, c, y], sm.at[d - 1], rm_sem.at[d - 1], tok=at_y(d))
    mb[z, c, y] = rm[y]

    def share_columns(d):
        got = nz.at[at_z(-d), y]
        for e in range(1, NY):
            send(got, got, sy.at[d, e - 1], ry.at[d, e - 1], tok=at_y(e))

    share_columns(0)

    sq = rows.astype(jnp.float32)
    sq = jnp.sum((sq * sq).reshape(64, 8, TG), axis=0)
    sq = sq[:, :128] + sq[:, 128:256] + sq[:, 256:]

    stages = [
        [dict(c=1 - c)],
        [dict(x=at_x(d)) for d in range(1, NX)],
        [dict(tok=at_y(d)) for d in range(1, NY)],
        [dict(z=at_z(d)) for d in range(1, NZ)],
    ]
    base = [0, 1, 4, 7]

    def trace_send(k):
        for i, where in enumerate(stages[k]):
            j = base[k] + i
            send(ts.at[k], trx.at[j], st.at[j], rt.at[j], **where)

    def trace_take(k):
        total = ts[k]
        for i in range(len(stages[k])):
            j = base[k] + i
            arrived(trx.at[j], rt.at[j])
            total = total + trx[j]
        return total

    ts[0] = sq
    trace_send(0)

    for d in range(1, NY):
        arrived(mb.at[z, c, at_y(-d)], rm_sem.at[d - 1])

    def ring(slot, s):
        if s < 4:
            send(mb.at[slot[0], c], mb.at[slot[0], c], sr.at[s - 1], rr.at[s - 1], z=at_z(1))
            send(mb.at[slot[1], c], mb.at[slot[1], c], sl.at[s - 1], rl.at[s - 1], z=at_z(-1))
        else:
            a, b = mb.at[slot[0], c, 0:2], mb.at[slot[1], c, 2:4]
            send(a, a, sr.at[s - 1], rr.at[s - 1], z=at_z(1))
            send(b, b, sl.at[s - 1], rl.at[s - 1], z=at_z(-1))

    def share(slot, k):
        got = mb.at[slot, c]
        send(got, got, sd.at[k], rd.at[k], c=1 - c)

    ring((z, z), 1)
    share(z, 0)

    for d in range(1, NZ):
        arrived(nz.at[at_z(-d), y], rn_sem.at[d - 1])
        share_columns(d)

    def ring_take(s):
        if s < 4:
            arrived(mb.at[at_z(-s), c], rr.at[s - 1])
            arrived(mb.at[at_z(s), c], rl.at[s - 1])
            ring((at_z(-s), at_z(s)), s + 1)
            share(at_z(-s), 2 * s - 1)
            share(at_z(s), 2 * s)
        else:
            arrived(mb.at[at_z(4), c, 0:2], rr.at[3])
            arrived(mb.at[at_z(4), c, 2:4], rl.at[3])
            share(at_z(4), 7)

    ring_take(1)
    ts[1] = trace_take(0)
    trace_send(1)

    order = column_order()
    for d in range(NZ):
        for e in range(1, NY):
            arrived(nz.at[at_z(-d), at_y(-e)], ry.at[d, e - 1])
    for j in range(NX):
        for e in range(NY):
            part = nz[:, e, j * 16 : (j + 1) * 16, :].reshape(128, TG)
            np_[j * 128 : (j + 1) * 128, e * TG : (e + 1) * TG] = lax.dot_general(
                order, part, NN, preferred_element_type=jnp.float32
            ).astype(jnp.bfloat16)

    slots = [z, at_z(-1), at_z(1), at_z(-2), at_z(2), at_z(-3), at_z(3), at_z(4)]
    right, left = at_x(1), at_x(-1)

    def multiply(k):
        slot = slots[k]
        arrived(mb.at[slot, 1 - c], rd.at[k])
        lhs = jnp.concatenate(
            [
                jnp.concatenate([mb[slot, e, f] for f in range(NY)], axis=1)
                for e in range(NC)
            ],
            axis=0,
        )
        prod = lax.dot_general(lhs, np_[...], NT, preferred_element_type=jnp.float32)
        for j in range(NX):
            g[k, j] = prod[:, j * 128 : (j + 1) * 128]
        far = g.at[k, at_x(2)]
        send(far.at[0:128], ra.at[k, 0], sa.at[k, 0], ra_sem.at[k, 0], x=right)
        send(far.at[128:256], ra.at[k, 1], sa.at[k, 1], ra_sem.at[k, 1], x=left)

    def pass_on(k):
        arrived(ra.at[k, 0], ra_sem.at[k, 0])
        g[k, right, 0:128, :] = g[k, right, 0:128, :] + ra[k, 0]
        send(g.at[k, right], rb.at[k, 0], sb.at[k, 0], rb_sem.at[k, 0], x=right)
        arrived(ra.at[k, 1], ra_sem.at[k, 1])
        g[k, left, 128:256, :] = g[k, left, 128:256, :] + ra[k, 1]
        send(g.at[k, left], rb.at[k, 1], sb.at[k, 1], rb_sem.at[k, 1], x=left)

    def finish(k):
        arrived(rb.at[k, 0], rb_sem.at[k, 0])
        arrived(rb.at[k, 1], rb_sem.at[k, 1])
        total = g[k, x] + rb[k, 0] + rb[k, 1]
        for i in range(32):
            start = (i >> 2) * 32 + (i & 3) + slots[k] * 4
            out[pl.ds(start, 8, stride=256), :] = total[i * 8 : (i + 1) * 8, :]

    multiply(0)
    multiply(1)
    pass_on(0)
    multiply(2)
    pass_on(1)
    ring_take(2)
    ts[2] = trace_take(1)
    trace_send(2)
    finish(0)
    multiply(3)
    pass_on(2)
    finish(1)
    multiply(4)
    pass_on(3)
    finish(2)
    ring_take(3)
    ts[3] = trace_take(2)
    trace_send(3)
    multiply(5)
    pass_on(4)
    finish(3)
    multiply(6)
    pass_on(5)
    finish(4)
    ring_take(4)
    multiply(7)
    pass_on(6)
    finish(5)
    tr[...] = trace_take(3)
    pass_on(7)
    finish(6)
    finish(7)
    for cp in started:
        cp.wait_send()


def rotate_and_multiply(picked, hs):
    bf, f32 = jnp.bfloat16, jnp.float32
    V = pltpu.VMEM
    dma = pltpu.SemaphoreType.DMA
    scratch = [
        V((NX, 128, TG), bf),
        V((NX, 128, TG), bf),
        V((NC, NZ, NX, 16, TG), bf),
        V((512, 1024), bf),
        V((512, 1024), bf),
        V((NY, 128, TG), bf),
        V((NZ, 64, TG), bf),
        V((NZ, NC, NY, 128, TG), bf),
        V((NZ, NY, 64, TG), bf),
        V((512, NY * TG), bf),
        V((NZ, NX, 256, 128), f32),
        V((NZ, 2, 128, 128), f32),
        V((NZ, 2, 256, 128), f32),
        V((4, 8, 128), f32),
        V((14, 8, 128), f32),
        dma((3,)), dma((3,)), dma((7,)), dma((7,)), dma((8,)), dma((8,)),
        dma((7,)), dma((7,)), dma((3,)), dma((3,)), dma((8, 3)), dma((8, 3)),
        dma((4,)), dma((4,)), dma((4,)), dma((4,)), dma((8,)), dma((8,)),
        dma((8, 2)), dma((8, 2)), dma((8, 2)), dma((8, 2)), dma((14,)), dma((14,)),
    ]
    vmem = pl.BlockSpec(memory_space=pltpu.VMEM)
    return pl.pallas_call(
        kernel,
        out_shape=(
            jax.ShapeDtypeStruct((2048, 128), f32),
            jax.ShapeDtypeStruct((8, 128), f32),
        ),
        in_specs=[vmem, vmem],
        out_specs=(vmem, vmem),
        scratch_shapes=scratch,
        compiler_params=pltpu.CompilerParams(
            collective_id=0, has_side_effects=True, vmem_limit_bytes=48 * 1024 * 1024
        ),
    )(picked, hs)


def shards(row_bank, token_ids, sign_flips, damping):
    picked = row_bank.at[token_ids].get(mode="promise_in_bounds")
    hs = (jnp.asarray(inner_table()) * sign_flips.astype(jnp.float32)[None, :]).astype(
        jnp.bfloat16
    )
    gram, squares = rotate_and_multiply(picked, hs)
    mean_diag = jnp.sum(squares) / TOKENS / D
    row_index = lax.axis_index("tok") * 2048 + lax.broadcasted_iota(jnp.int32, gram.shape, 0)
    col_index = lax.axis_index(COL) * 128 + lax.broadcasted_iota(jnp.int32, gram.shape, 1)
    on_diag = (row_index == col_index).astype(jnp.float32)
    return gram / TOKENS + damping[0] * mean_diag * on_diag


def solution(mesh):
    split = Mesh(mesh.devices.reshape(NY, NZ, NX, NC), ("tok",) + COL)
    return jax.shard_map(
        shards,
        mesh=split,
        in_specs=(P(None, COL), P("tok"), P(COL), P()),
        out_specs=P("tok", COL),
        check_vma=False,
    )
```

```python
import functools
import math

import jax
import jax.numpy as jnp
import numpy as np
from jax import lax
from jax.experimental import pallas as pl
from jax.experimental.pallas import tpu as pltpu
from jax.sharding import Mesh
from jax.sharding import PartitionSpec as P

D = 8192
BLOCK = 32
TOKENS = 6144
COL = ("z", "x", "c")
NY, NZ, NX, NC = 4, 8, 4, 2
TG = TOKENS // (NY * NX)
TT = 128
NT3 = TG // TT
HOPS = (4, 1, 7, 2, 6, 3, 5)
MESH = pl.DeviceIdType.MESH
NT = (((1,), (1,)), ((), ()))
NN = (((1,), (0,)), ((), ()))


def parity_sign(v):
    v = v ^ (v >> 4)
    v = v ^ (v >> 2)
    v = v ^ (v >> 1)
    return 1 - 2 * (v & 1)


def inner_table():
    r = np.arange(128)
    b_r, a_r = (r >> 4) * 4 + (r & 3), (r >> 2) & 3
    b_c, a_c = r & 31, r >> 5
    bits = np.array([bin(i).count("1") & 1 for i in range(32)])
    signs = 1 - 2 * bits[b_r[:, None] & b_c[None, :]]
    return np.where(a_r[:, None] == a_c[None, :], signs, 0).astype(np.float32)


def outer_table(core, for_rows):
    r = lax.broadcasted_iota(jnp.int32, (512, 1), 0)
    k = lax.broadcasted_iota(jnp.int32, (1, 1024), 1)
    if for_rows:
        c = ((r >> 7) << 6) | ((r & 7) << 3) | ((r >> 5) & 3)
        b_r = (r >> 3) & 3
    else:
        c = ((r >> 6) << 5) | (((r >> 4) & 3) << 3) | ((r >> 2) & 3)
        b_r = r & 3
    c = c | (core << 2)
    a = (((k >> 6) & 7) << 5) | (((k >> 4) & 3) << 3) | ((k >> 9) << 2) | ((k >> 2) & 3)
    sign = parity_sign(c & a)
    return jnp.where(b_r == (k & 3), sign, 0).astype(jnp.float32).astype(jnp.bfloat16)


def column_order():
    o = lax.broadcasted_iota(jnp.int32, (128, 128), 0)
    i = lax.broadcasted_iota(jnp.int32, (128, 128), 1)
    src = (((o >> 2) & 7) << 4) | ((o >> 5) << 2) | (o & 3)
    return (i == src).astype(jnp.float32).astype(jnp.bfloat16)


def kernel(
    picked, hs, signs, out, tr,
    hb, x1, x2, hm, hn, rm, rn, mb, nz, np_, g, ra, rb, ts, trx,
    s1, r1, s2, r2, s3, r3, sn, rn_sem, sm, rm_sem, sy, ry, sr, rr, sl, rl, sd, rd,
    sa, ra_sem, sb, rb_sem, st, rt,
):
    y, z, x, c = (lax.axis_index(n) for n in ("tok", "z", "x", "c"))
    scale = 1.0 / math.sqrt(D)

    def at_x(d):
        return lax.rem(x + d + NX, NX)

    def at_y(d):
        return lax.rem(y + d + NY, NY)

    def at_z(d):
        return lax.rem(z + d + NZ, NZ)

    def copy(src, dst, send, recv, **where):
        return pltpu.make_async_remote_copy(
            src_ref=src, dst_ref=dst, send_sem=send, recv_sem=recv,
            device_id=where, device_id_type=MESH,
        )

    started = []

    def send(*args, **where):
        cp = copy(*args, **where)
        cp.start()
        started.append(cp)

    def arrived(ref, sem):
        copy(ref, ref, sem, sem, c=1 - c).wait_recv()

    barrier = pltpu.get_barrier_semaphore()
    peers = (
        [dict(x=at_x(d)) for d in range(1, NX)]
        + [dict(tok=at_y(d)) for d in range(1, NY)]
        + [dict(z=at_z(d)) for d in range(1, NZ)]
        + [dict(c=1 - c)]
    )
    for where in peers:
        pl.semaphore_signal(barrier, inc=1, device_id=where, device_id_type=MESH)

    signed = (hs[...] * signs[...].astype(jnp.float32)).astype(jnp.bfloat16)
    for t in range(NT3):
        for j in range(NX):
            first = j * TG + t * TT
            h = lax.dot_general(
                signed, picked[first : first + TT, :], NT, preferred_element_type=jnp.float32
            )
            hb[t, j] = h.astype(jnp.bfloat16)
        if t == 0:
            pl.semaphore_wait(barrier, len(peers))
        for d in range(1, NX):
            send(hb.at[t, at_x(d)], x1.at[t, x], s1.at[t, d - 1], r1.at[t, d - 1], x=at_x(d))
        x1[t, x] = hb[t, x]
    hn[...] = outer_table(c, False)

    def piece(t, zz):
        return x1.at[t, :, pl.ds(pl.multiple_of(zz * 16, 16), 16), :]

    for t in range(NT3):
        for d in range(1, NX):
            arrived(x1.at[t, at_x(-d)], r1.at[t, d - 1])
        for d in HOPS:
            send(piece(t, at_z(d)), x2.at[t, c, z], s2.at[t, d - 1], r2.at[t, d - 1], z=at_z(d))
        send(piece(t, z), x2.at[t, c, z], s3.at[t, 0], r3.at[t, 0], c=1 - c)
        x2[t, c, z] = x1[t, :, pl.ds(pl.multiple_of(z * 16, 16), 16), :]
    hm[...] = outer_table(c, True)

    def share_turned(t):
        for d in HOPS:
            got = x2.at[t, c, at_z(-d)]
            arrived(got, r2.at[t, d - 1])
            send(got, got, s3.at[t, d], r3.at[t, d], c=1 - c)

    def turn(t):
        for d in range(NZ):
            arrived(x2.at[t, 1 - c, at_z(-d)], r3.at[t, d])
        spread = x2[t].reshape(1024, TT)

        def times(table):
            return (
                lax.dot_general(table[...], spread, NN, preferred_element_type=jnp.float32) * scale
            ).astype(jnp.bfloat16)

        rn[t] = times(hn).reshape(NZ, 64, TT)
        for d in HOPS:
            send(
                rn.at[t, at_z(d)], nz.at[z, y, t], sn.at[t, d - 1], rn_sem.at[t, d - 1], z=at_z(d)
            )
        nz[z, y, t] = rn[t, z]
        rows = times(hm)
        rm[t] = rows.reshape(NY, 128, TT)
        for d in range(1, NY):
            send(
                rm.at[t, at_y(d)], mb.at[z, c, y, t], sm.at[t, d - 1], rm_sem.at[t, d - 1],
                tok=at_y(d),
            )
        mb[z, c, y, t] = rm[t, y]
        sq = rows.astype(jnp.float32)
        return jnp.sum((sq * sq).reshape(64, 8, TT), axis=0)

    def near(t, d):
        got = nz.at[at_z(-d), y, t]
        send(got, got, sy.at[t, d, 0], ry.at[t, d, 0], tok=at_y(1))
        send(got, got, sy.at[t, d, 1], ry.at[t, d, 1], tok=at_y(-1))

    def far(t, d):
        left, right = nz.at[at_z(-d), at_y(-1), t], nz.at[at_z(-d), at_y(1), t]
        arrived(left, ry.at[t, d, 0])
        arrived(right, ry.at[t, d, 1])
        if (t + d) % 2 == 0:
            send(left, left, sy.at[t, d, 2], ry.at[t, d, 2], tok=at_y(1))
        else:
            send(right, right, sy.at[t, d, 2], ry.at[t, d, 2], tok=at_y(-1))

    stages = [
        [dict(c=1 - c)],
        [dict(x=at_x(d)) for d in range(1, NX)],
        [dict(tok=at_y(d)) for d in range(1, NY)],
        [dict(z=at_z(d)) for d in range(1, NZ)],
    ]
    base = [0, 1, 4, 7]

    def trace_send(k):
        for i, where in enumerate(stages[k]):
            j = base[k] + i
            send(ts.at[k], trx.at[j], st.at[j], rt.at[j], **where)

    def trace_take(k):
        total = ts[k]
        for i in range(len(stages[k])):
            j = base[k] + i
            arrived(trx.at[j], rt.at[j])
            total = total + trx[j]
        return total

    def ring(slot, s):
        if s < 4:
            send(mb.at[slot[0], c], mb.at[slot[0], c], sr.at[s - 1], rr.at[s - 1], z=at_z(1))
            send(mb.at[slot[1], c], mb.at[slot[1], c], sl.at[s - 1], rl.at[s - 1], z=at_z(-1))
        else:
            a, b = mb.at[slot[0], c, 0:2], mb.at[slot[1], c, 2:4]
            send(a, a, sr.at[s - 1], rr.at[s - 1], z=at_z(1))
            send(b, b, sl.at[s - 1], rl.at[s - 1], z=at_z(-1))

    def share(slot, k):
        got = mb.at[slot, c]
        send(got, got, sd.at[k], rd.at[k], c=1 - c)

    def ring_take(s):
        if s < 4:
            arrived(mb.at[at_z(-s), c], rr.at[s - 1])
            arrived(mb.at[at_z(s), c], rl.at[s - 1])
            ring((at_z(-s), at_z(s)), s + 1)
            share(at_z(-s), 2 * s - 1)
            share(at_z(s), 2 * s)
        else:
            arrived(mb.at[at_z(4), c, 0:2], rr.at[3])
            arrived(mb.at[at_z(4), c, 2:4], rl.at[3])
            share(at_z(4), 7)

    share_turned(0)
    share_turned(1)
    sq = turn(0)
    share_turned(2)
    sq = sq + turn(1)
    sq = sq + turn(2)
    ts[0] = sq
    trace_send(0)
    for t in range(NT3):
        near(t, 0)
        for d in range(1, NY):
            arrived(mb.at[z, c, at_y(-d), t], rm_sem.at[t, d - 1])
    ring((z, z), 1)
    share(z, 0)
    for t in range(NT3):
        for d in HOPS:
            arrived(nz.at[at_z(-d), y, t], rn_sem.at[t, d - 1])
            near(t, d)
        if t == 0:
            for e in range(NT3):
                far(e, 0)
        else:
            for d in HOPS:
                far(t - 1, d)
    for d in HOPS:
        far(NT3 - 1, d)
    ts[1] = trace_take(0)
    trace_send(1)

    order = column_order()
    for t in range(NT3):
        for d in range(NZ):
            arrived(nz.at[at_z(-d), at_y(2), t], ry.at[t, d, 2])
        for e in range(NY):
            lane = e * TG + t * TT
            for j in range(NX):
                part = nz[:, e, t, j * 16 : (j + 1) * 16, :].reshape(128, TT)
                np_[j * 128 : (j + 1) * 128, lane : lane + TT] = lax.dot_general(
                    order, part, NN, preferred_element_type=jnp.float32
                ).astype(jnp.bfloat16)
    ring_take(1)

    slots = [z, at_z(-1), at_z(1), at_z(-2), at_z(2), at_z(-3), at_z(3), at_z(4)]
    right, left = at_x(1), at_x(-1)

    def multiply(k):
        slot = slots[k]
        arrived(mb.at[slot, 1 - c], rd.at[k])
        lhs = jnp.concatenate(
            [
                jnp.concatenate(
                    [mb[slot, e, f, t] for f in range(NY) for t in range(NT3)], axis=1
                )
                for e in range(NC)
            ],
            axis=0,
        )
        prod = lax.dot_general(lhs, np_[...], NT, preferred_element_type=jnp.float32)
        for j in range(NX):
            g[k, j] = prod[:, j * 128 : (j + 1) * 128]
        far = g.at[k, at_x(2)]
        send(far.at[0:128], ra.at[k, 0], sa.at[k, 0], ra_sem.at[k, 0], x=right)
        send(far.at[128:256], ra.at[k, 1], sa.at[k, 1], ra_sem.at[k, 1], x=left)

    def pass_on(k):
        arrived(ra.at[k, 0], ra_sem.at[k, 0])
        g[k, right, 0:128, :] = g[k, right, 0:128, :] + ra[k, 0]
        send(g.at[k, right], rb.at[k, 0], sb.at[k, 0], rb_sem.at[k, 0], x=right)
        arrived(ra.at[k, 1], ra_sem.at[k, 1])
        g[k, left, 128:256, :] = g[k, left, 128:256, :] + ra[k, 1]
        send(g.at[k, left], rb.at[k, 1], sb.at[k, 1], rb_sem.at[k, 1], x=left)

    def finish(k):
        arrived(rb.at[k, 0], rb_sem.at[k, 0])
        arrived(rb.at[k, 1], rb_sem.at[k, 1])
        total = g[k, x] + rb[k, 0] + rb[k, 1]
        for i in range(32):
            start = (i >> 2) * 32 + (i & 3) + slots[k] * 4
            out[pl.ds(start, 8, stride=256), :] = total[i * 8 : (i + 1) * 8, :]

    multiply(0)
    multiply(1)
    pass_on(0)
    multiply(2)
    pass_on(1)
    ring_take(2)
    ts[2] = trace_take(1)
    trace_send(2)
    finish(0)
    multiply(3)
    pass_on(2)
    finish(1)
    multiply(4)
    pass_on(3)
    finish(2)
    ring_take(3)
    ts[3] = trace_take(2)
    trace_send(3)
    multiply(5)
    pass_on(4)
    finish(3)
    multiply(6)
    pass_on(5)
    finish(4)
    ring_take(4)
    multiply(7)
    pass_on(6)
    finish(5)
    tr[...] = jnp.full((8, 128), jnp.sum(trace_take(3)), jnp.float32)
    pass_on(7)
    finish(6)
    finish(7)
    for cp in started:
        cp.wait_send()


def rotate_and_multiply(picked, hs, signs):
    bf, f32 = jnp.bfloat16, jnp.float32
    V = pltpu.VMEM
    dma = pltpu.SemaphoreType.DMA
    scratch = [
        V((NT3, NX, 128, TT), bf),
        V((NT3, NX, 128, TT), bf),
        V((NT3, NC, NZ, NX, 16, TT), bf),
        V((512, 1024), bf),
        V((512, 1024), bf),
        V((NT3, NY, 128, TT), bf),
        V((NT3, NZ, 64, TT), bf),
        V((NZ, NC, NY, NT3, 128, TT), bf),
        V((NZ, NY, NT3, 64, TT), bf),
        V((512, NY * TG), bf),
        V((NZ, NX, 256, 128), f32),
        V((NZ, 2, 128, 128), f32),
        V((NZ, 2, 256, 128), f32),
        V((4, 8, 128), f32),
        V((14, 8, 128), f32),
    ] + [
        dma(shape)
        for shape in (
            (NT3, 3), (NT3, 7), (NT3, 8), (NT3, 7), (NT3, 3), (NT3, 8, 3),
            (4,), (4,), (8,), (8, 2), (8, 2), (14,),
        )
        for _ in range(2)
    ]
    vmem = pl.BlockSpec(memory_space=pltpu.VMEM)
    return pl.pallas_call(
        kernel,
        out_shape=(
            jax.ShapeDtypeStruct((2048, 128), f32),
            jax.ShapeDtypeStruct((8, 128), f32),
        ),
        in_specs=[vmem, vmem, vmem],
        out_specs=(vmem, vmem),
        scratch_shapes=scratch,
        compiler_params=pltpu.CompilerParams(
            collective_id=0, has_side_effects=True, vmem_limit_bytes=48 * 1024 * 1024
        ),
    )(picked, hs, signs)


def shards(row_bank, token_ids, sign_flips, damping):
    picked = lax.gather(
        row_bank,
        token_ids[:, None],
        lax.GatherDimensionNumbers((1,), (0,), (0,)),
        (1, row_bank.shape[1]),
        mode=lax.GatherScatterMode.PROMISE_IN_BOUNDS,
    )
    gram, squares = rotate_and_multiply(picked, jnp.asarray(inner_table()), sign_flips[None, :])
    mean_diag = squares[0, 0] / TOKENS / D
    row_index = lax.axis_index("tok") * 2048 + lax.broadcasted_iota(jnp.int32, gram.shape, 0)
    col_index = lax.axis_index(COL) * 128 + lax.broadcasted_iota(jnp.int32, gram.shape, 1)
    on_diag = (row_index == col_index).astype(jnp.float32)
    return gram / TOKENS + damping[0] * mean_diag * on_diag


def solution(mesh):
    split = Mesh(mesh.devices.reshape(NY, NZ, NX, NC), ("tok",) + COL)
    return jax.shard_map(
        shards,
        mesh=split,
        in_specs=(P(None, COL), P("tok"), P(COL), P()),
        out_specs=P("tok", COL),
        check_vma=False,
    )
```

```python
import math

import jax
import jax.numpy as jnp
from jax import lax
from jax.experimental import pallas as pl
from jax.experimental.pallas import tpu as pltpu
from jax.sharding import Mesh
from jax.sharding import PartitionSpec as P

D = 8192
BLOCK = 32
TOKENS = 6144
COL = ("z", "x", "c")
NY, NZ, NX, NC = 4, 8, 4, 2
TG = TOKENS // (NY * NX)
TT = 128
NT3 = TG // TT
HOPS = (4, 1, 7, 2, 6, 3, 5)
MESH = pl.DeviceIdType.MESH
NT = (((1,), (1,)), ((), ()))
NN = (((1,), (0,)), ((), ()))


def parity_sign(v):
    v = v ^ (v >> 4)
    v = v ^ (v >> 2)
    v = v ^ (v >> 1)
    return 1 - 2 * (v & 1)


def inner_table():
    r = lax.broadcasted_iota(jnp.int32, (128, 128), 0)
    k = lax.broadcasted_iota(jnp.int32, (128, 128), 1)
    b_r = ((r >> 4) << 2) | (r & 3)
    sign = parity_sign(b_r & (k & 31))
    return jnp.where(((r >> 2) & 3) == (k >> 5), sign, 0)


def outer_table(core, for_rows):
    r = lax.broadcasted_iota(jnp.int32, (512, 1), 0)
    k = lax.broadcasted_iota(jnp.int32, (1, 1024), 1)
    if for_rows:
        c = ((r >> 7) << 6) | ((r & 7) << 3) | ((r >> 5) & 3)
        b_r = (r >> 3) & 3
    else:
        c = ((r >> 6) << 5) | (((r >> 4) & 3) << 3) | ((r >> 2) & 3)
        b_r = r & 3
    c = c | (core << 2)
    a = (((k >> 4) & 7) << 5) | (((k >> 7) & 3) << 3) | ((k >> 9) << 2) | ((k >> 2) & 3)
    sign = parity_sign(c & a)
    return jnp.where(b_r == (k & 3), sign, 0).astype(jnp.float32).astype(jnp.bfloat16)


def column_order():
    o = lax.broadcasted_iota(jnp.int32, (128, 128), 0)
    i = lax.broadcasted_iota(jnp.int32, (128, 128), 1)
    src = (((o >> 2) & 7) << 4) | ((o >> 5) << 2) | (o & 3)
    return (i == src).astype(jnp.float32).astype(jnp.bfloat16)


def kernel(
    picked, signs_any, out, tr,
    signs, signs_sem, hb, x1, x2, hm, hn, rm, rn, mb, nz, np_, g, ra, rb, ts, trx,
    s1, r1, s2, r2, s3, r3, sn, rn_sem, sm, rm_sem, sy, ry, sr, rr, sl, rl, sd, rd,
    sa, ra_sem, sb, rb_sem, st, rt,
):
    y, z, x, c = (lax.axis_index(n) for n in ("tok", "z", "x", "c"))
    scale = 1.0 / math.sqrt(D)

    def at_x(d):
        return lax.rem(x + d + NX, NX)

    def at_y(d):
        return lax.rem(y + d + NY, NY)

    def at_z(d):
        return lax.rem(z + d + NZ, NZ)

    def copy(src, dst, send, recv, **where):
        return pltpu.make_async_remote_copy(
            src_ref=src, dst_ref=dst, send_sem=send, recv_sem=recv,
            device_id=where, device_id_type=MESH,
        )

    started = []

    def send(*args, **where):
        cp = copy(*args, **where)
        cp.start()
        started.append(cp)

    def arrived(ref, sem):
        copy(ref, ref, sem, sem, c=1 - c).wait_recv()

    barrier = pltpu.get_barrier_semaphore()
    peers = (
        [dict(x=at_x(d)) for d in range(1, NX)]
        + [dict(tok=at_y(d)) for d in range(1, NY)]
        + [dict(z=at_z(d)) for d in range(1, NZ)]
        + [dict(c=1 - c)]
    )
    for where in peers:
        pl.semaphore_signal(barrier, inc=1, device_id=where, device_id_type=MESH)

    fetch = pltpu.make_async_copy(signs_any, signs, signs_sem)
    fetch.start()
    table = inner_table()
    fetch.wait()
    signed = (table * signs[...]).astype(jnp.float32).astype(jnp.bfloat16)

    def piece(t, zz):
        return hb.at[t, :, pl.ds(pl.multiple_of(zz * 16, 16), 16), :]

    for t in range(NT3):
        for j in range(NX):
            first = j * TG + t * TT
            h = lax.dot_general(
                signed, picked[first : first + TT, :], NT, preferred_element_type=jnp.float32
            )
            hb[t, j] = h.astype(jnp.bfloat16)
        if t == 0:
            pl.semaphore_wait(barrier, len(peers))
        for d in HOPS:
            send(piece(t, at_z(d)), x1.at[t, z], s2.at[t, d - 1], r2.at[t, d - 1], z=at_z(d))
        x1[t, z] = hb[t, :, pl.ds(pl.multiple_of(z * 16, 16), 16), :]
    hn[...] = outer_table(c, False)
    hm[...] = outer_table(c, True)

    def exchange(t):
        for d in HOPS:
            arrived(x1.at[t, at_z(-d)], r2.at[t, d - 1])
        for d in (2, 1, 3):
            send(
                x1.at[t, :, at_x(d)], x2.at[t, c, x], s1.at[t, d - 1], r1.at[t, d - 1], x=at_x(d)
            )
        send(x1.at[t, :, x], x2.at[t, c, x], s3.at[t, 0], r3.at[t, 0], c=1 - c)
        x2[t, c, x] = x1[t, :, x]

    def share_turned(t):
        for d in (1, 3, 2):
            got = x2.at[t, c, at_x(-d)]
            arrived(got, r1.at[t, d - 1])
            send(got, got, s3.at[t, d], r3.at[t, d], c=1 - c)

    def turn(t):
        for d in range(NX):
            arrived(x2.at[t, 1 - c, at_x(-d)], r3.at[t, d])
        spread = x2[t].reshape(1024, TT)

        def times(table):
            return (
                lax.dot_general(table[...], spread, NN, preferred_element_type=jnp.float32) * scale
            ).astype(jnp.bfloat16)

        rn[t] = times(hn).reshape(NZ, 64, TT)
        for d in HOPS:
            send(
                rn.at[t, at_z(d)], nz.at[z, y, t], sn.at[t, d - 1], rn_sem.at[t, d - 1], z=at_z(d)
            )
        nz[z, y, t] = rn[t, z]
        rows = times(hm)
        rm[t] = rows.reshape(NY, 128, TT)
        for d in range(1, NY):
            send(
                rm.at[t, at_y(d)], mb.at[z, c, y, t], sm.at[t, d - 1], rm_sem.at[t, d - 1],
                tok=at_y(d),
            )
        mb[z, c, y, t] = rm[t, y]
        sq = rows.astype(jnp.float32)
        return jnp.sum((sq * sq).reshape(64, 8, TT), axis=0)

    def near(t, d):
        got = nz.at[at_z(-d), y, t]
        send(got, got, sy.at[t, d, 0], ry.at[t, d, 0], tok=at_y(1))
        send(got, got, sy.at[t, d, 1], ry.at[t, d, 1], tok=at_y(-1))

    def far(t, d):
        left, right = nz.at[at_z(-d), at_y(-1), t], nz.at[at_z(-d), at_y(1), t]
        arrived(left, ry.at[t, d, 0])
        arrived(right, ry.at[t, d, 1])
        if (t + d) % 2 == 0:
            send(left, left, sy.at[t, d, 2], ry.at[t, d, 2], tok=at_y(1))
        else:
            send(right, right, sy.at[t, d, 2], ry.at[t, d, 2], tok=at_y(-1))

    stages = [
        [dict(c=1 - c)],
        [dict(x=at_x(d)) for d in range(1, NX)],
        [dict(tok=at_y(d)) for d in range(1, NY)],
        [dict(z=at_z(d)) for d in range(1, NZ)],
    ]
    base = [0, 1, 4, 7]

    def trace_send(k):
        for i, where in enumerate(stages[k]):
            j = base[k] + i
            send(ts.at[k], trx.at[j], st.at[j], rt.at[j], **where)

    def trace_take(k):
        total = ts[k]
        for i in range(len(stages[k])):
            j = base[k] + i
            arrived(trx.at[j], rt.at[j])
            total = total + trx[j]
        return total

    def ring(back, ahead, s, e):
        f = at_y(-e)
        if s < 4 or e < 2:
            got = mb.at[back, c, f]
            send(got, got, sr.at[s - 1, e], rr.at[s - 1, e], z=at_z(1))
        if s < 4 or e >= 2:
            got = mb.at[ahead, c, f]
            send(got, got, sl.at[s - 1, e], rl.at[s - 1, e], z=at_z(-1))

    def share(slot, k, e):
        got = mb.at[slot, c, at_y(-e)]
        send(got, got, sd.at[k, e], rd.at[k, e], c=1 - c)

    def ring_take(s, e):
        back, ahead, f = at_z(-s), at_z(s), at_y(-e)
        if s < 4 or e < 2:
            arrived(mb.at[back, c, f], rr.at[s - 1, e])
        if s < 4 or e >= 2:
            arrived(mb.at[ahead, c, f], rl.at[s - 1, e])
        if s < 4:
            ring(back, ahead, s + 1, e)
            share(back, 2 * s - 1, e)
            share(ahead, 2 * s, e)
        else:
            share(back, 7, e)

    exchange(0)
    exchange(1)
    share_turned(0)
    exchange(2)
    sq = turn(0)
    share_turned(1)
    sq = sq + turn(1)
    near(0, 0)
    share_turned(2)
    sq = sq + turn(2)
    near(1, 0)
    near(2, 0)
    ts[0] = sq
    trace_send(0)
    for e in range(NY):
        if e:
            for t in range(NT3):
                arrived(mb.at[z, c, at_y(-e), t], rm_sem.at[t, e - 1])
        ring(z, z, 1, e)
        share(z, 0, e)
    for t in range(NT3):
        for d in HOPS:
            arrived(nz.at[at_z(-d), y, t], rn_sem.at[t, d - 1])
            near(t, d)
        if t == 0:
            for e in range(NT3):
                far(e, 0)
        else:
            for d in HOPS:
                far(t - 1, d)
    ring_take(1, 0)
    for d in HOPS:
        far(NT3 - 1, d)
    ts[1] = trace_take(0)
    trace_send(1)
    ring_take(1, 1)

    order = column_order()
    for t in range(NT3):
        for d in range(NZ):
            arrived(nz.at[at_z(-d), at_y(2), t], ry.at[t, d, 2])
        for e in range(NY):
            lane = e * TG + t * TT
            for j in range(NX):
                part = nz[:, e, t, j * 16 : (j + 1) * 16, :].reshape(128, TT)
                np_[j * 128 : (j + 1) * 128, lane : lane + TT] = lax.dot_general(
                    order, part, NN, preferred_element_type=jnp.float32
                ).astype(jnp.bfloat16)

    slots = [z, at_z(-1), at_z(1), at_z(-2), at_z(2), at_z(-3), at_z(3), at_z(4)]
    right, left = at_x(1), at_x(-1)

    def multiply(k):
        slot = slots[k]
        for e in range(NY):
            arrived(mb.at[slot, 1 - c, at_y(-e)], rd.at[k, e])
        lhs = jnp.concatenate(
            [
                jnp.concatenate(
                    [mb[slot, e, f, t] for f in range(NY) for t in range(NT3)], axis=1
                )
                for e in range(NC)
            ],
            axis=0,
        )
        prod = lax.dot_general(lhs, np_[...], NT, preferred_element_type=jnp.float32)
        for j in range(NX):
            g[k, j] = prod[:, j * 128 : (j + 1) * 128]
        apart = g.at[k, at_x(2)]
        send(apart.at[0:128], ra.at[k, 0], sa.at[k, 0], ra_sem.at[k, 0], x=right)
        send(apart.at[128:256], ra.at[k, 1], sa.at[k, 1], ra_sem.at[k, 1], x=left)
        hand(k, 0, 1)
        hand(k, 1, 0)

    def hand(k, side, half):
        to = (right, left)[side]
        src = g.at[k, to, half * 128 : half * 128 + 128]
        send(
            src, rb.at[k, side, half], sb.at[k, side, half], rb_sem.at[k, side, half], x=to
        )

    def pass_on(k):
        for side, to in ((0, right), (1, left)):
            arrived(ra.at[k, side], ra_sem.at[k, side])
            rows = slice(side * 128, side * 128 + 128)
            g[k, to, rows, :] = g[k, to, rows, :] + ra[k, side]
            hand(k, side, side)

    def finish(k):
        for half in (1, 0):
            arrived(rb.at[k, half, 1 - half], rb_sem.at[k, half, 1 - half])
        for half in range(2):
            arrived(rb.at[k, half, half], rb_sem.at[k, half, half])
        for half in range(2):
            rows = slice(half * 128, half * 128 + 128)
            total = g[k, x, rows, :] + rb[k, 0, half] + rb[k, 1, half]
            for i in range(16):
                start = half * 128 + (i >> 2) * 32 + (i & 3) + slots[k] * 4
                out[pl.ds(start, 8, stride=256), :] = total[i * 8 : (i + 1) * 8, :]

    multiply(0)
    ring_take(1, 2)
    ring_take(1, 3)
    multiply(1)
    pass_on(0)
    multiply(2)
    for s in range(1, 4):
        ring_take(s + 1, 0)
        pass_on(2 * s - 1)
        ring_take(s + 1, 1)
        if s == 1:
            finish(0)
        pass_on(2 * s)
        ring_take(s + 1, 2)
        finish(2 * s - 1)
        ring_take(s + 1, 3)
        multiply(2 * s + 1)
        if s < 3:
            multiply(2 * s + 2)
            ts[s + 1] = trace_take(s)
            trace_send(s + 1)
        finish(2 * s)
    pass_on(7)
    tr[...] = jnp.full((8, 128), jnp.sum(trace_take(3)), jnp.float32)
    finish(7)
    for cp in started:
        cp.wait_send()


def rotate_and_multiply(picked, signs):
    bf, f32 = jnp.bfloat16, jnp.float32
    V = pltpu.VMEM
    dma = pltpu.SemaphoreType.DMA
    scratch = [
        V((1, 128), jnp.int32),
        dma(()),
        V((NT3, NX, 128, TT), bf),
        V((NT3, NZ, NX, 16, TT), bf),
        V((NT3, NC, NX, NZ, 16, TT), bf),
        V((512, 1024), bf),
        V((512, 1024), bf),
        V((NT3, NY, 128, TT), bf),
        V((NT3, NZ, 64, TT), bf),
        V((NZ, NC, NY, NT3, 128, TT), bf),
        V((NZ, NY, NT3, 64, TT), bf),
        V((512, NY * TG), bf),
        V((NZ, NX, 256, 128), f32),
        V((NZ, 2, 128, 128), f32),
        V((NZ, 2, 2, 128, 128), f32),
        V((4, 8, 128), f32),
        V((14, 8, 128), f32),
    ] + [
        dma(shape)
        for shape in (
            (NT3, 3), (NT3, 7), (NT3, 4), (NT3, 7), (NT3, 3), (NT3, 8, 3),
            (4, 4), (4, 4), (8, 4), (8, 2), (8, 2, 2), (14,),
        )
        for _ in range(2)
    ]
    vmem = pl.BlockSpec(memory_space=pltpu.VMEM)
    return pl.pallas_call(
        kernel,
        out_shape=(
            jax.ShapeDtypeStruct((2048, 128), f32),
            jax.ShapeDtypeStruct((8, 128), f32),
        ),
        in_specs=[vmem, pl.BlockSpec(memory_space=pltpu.MemorySpace.HBM)],
        out_specs=(vmem, vmem),
        scratch_shapes=scratch,
        compiler_params=pltpu.CompilerParams(
            collective_id=0, has_side_effects=True, vmem_limit_bytes=48 * 1024 * 1024
        ),
    )(picked, signs)


def shards(row_bank, token_ids, sign_flips, damping):
    picked = lax.gather(
        row_bank,
        token_ids[:, None],
        lax.GatherDimensionNumbers((1,), (0,), (0,)),
        (1, row_bank.shape[1]),
        mode=lax.GatherScatterMode.PROMISE_IN_BOUNDS,
    )
    gram, squares = rotate_and_multiply(picked, sign_flips[None, :])
    mean_diag = squares[:1, :] / TOKENS / D
    row_index = lax.axis_index("tok") * 2048 + lax.broadcasted_iota(jnp.int32, gram.shape, 0)
    col_index = lax.axis_index(COL) * 128 + lax.broadcasted_iota(jnp.int32, gram.shape, 1)
    on_diag = (row_index == col_index).astype(jnp.float32)
    return gram / TOKENS + damping[0] * mean_diag * on_diag


def solution(mesh):
    split = Mesh(mesh.devices.reshape(NY, NZ, NX, NC), ("tok",) + COL)
    return jax.shard_map(
        shards,
        mesh=split,
        in_specs=(P(None, COL), P("tok"), P(COL), P()),
        out_specs=P("tok", COL),
        check_vma=False,
    )
```

```python
import math

import jax
import jax.numpy as jnp
from jax import lax
from jax.experimental import pallas as pl
from jax.experimental.pallas import tpu as pltpu
from jax.sharding import Mesh
from jax.sharding import PartitionSpec as P

D = 8192
BLOCK = 32
TOKENS = 6144
COL = ("z", "x", "c")
NY, NZ, NX, NC = 4, 8, 4, 2
TG = TOKENS // (NY * NX)
TT = 128
NT3 = TG // TT
HOPS = (4, 3, 5, 2, 6, 1, 7)
TILES = (1, 2, 0)
MESH = pl.DeviceIdType.MESH
NT = (((1,), (1,)), ((), ()))
NN = (((1,), (0,)), ((), ()))


def parity_sign(v):
    v = v ^ (v >> 4)
    v = v ^ (v >> 2)
    v = v ^ (v >> 1)
    return 1 - 2 * (v & 1)


def inner_table():
    r = lax.broadcasted_iota(jnp.int32, (128, 128), 0)
    k = lax.broadcasted_iota(jnp.int32, (128, 128), 1)
    b_r = ((r >> 4) << 2) | (r & 3)
    sign = parity_sign(b_r & (k & 31))
    return jnp.where(((r >> 2) & 3) == (k >> 5), sign, 0)


def outer_table(core, for_rows):
    k = lax.broadcasted_iota(jnp.int32, (1, 1024), 1)
    a = (((k >> 4) & 7) << 5) | (((k >> 7) & 3) << 3) | ((k >> 9) << 2) | ((k >> 2) & 3)

    def bits(r):
        if for_rows:
            return ((r >> 7) << 6) | ((r & 7) << 3) | ((r >> 5) & 3), (r >> 3) & 3
        return ((r >> 6) << 5) | (((r >> 4) & 3) << 3) | ((r >> 2) & 3), r & 3

    c_group, b_group = bits(lax.broadcasted_iota(jnp.int32, (64, 1), 0) * 8)
    c_place, b_place = bits(lax.broadcasted_iota(jnp.int32, (8, 1), 0))
    group = parity_sign((c_group | (core << 2)) & a)
    place = parity_sign(c_place & a)
    if for_rows:
        group = jnp.where(b_group == (k & 3), group, 0)
    else:
        place = jnp.where(b_place == (k & 3), place, 0)
    group, place = group.astype(jnp.float32), place.astype(jnp.float32)
    table = group[:, None, :] * place[None, :, :]
    return table.reshape(512, 1024).astype(jnp.bfloat16)


def column_order():
    o = lax.broadcasted_iota(jnp.int32, (128, 128), 0)
    i = lax.broadcasted_iota(jnp.int32, (128, 128), 1)
    src = (((o >> 2) & 7) << 4) | ((o >> 5) << 2) | (o & 3)
    return (i == src).astype(jnp.float32).astype(jnp.bfloat16)


def kernel(
    damping, picked, signs_any, out,
    signs, signs_sem, xf, hb, x1, x2, hm, hn, rm, rn, mb, nz, np_, g, ra, rb, ts, trx,
    s1, r1, s2, r2, s3, r3, sn, rn_sem, sm, rm_sem, sy, ry, sr, rr, sl, rl, sd, rd,
    sa, ra_sem, sb, rb_sem, st, rt,
):
    y, z, x, c = (lax.axis_index(n) for n in ("tok", "z", "x", "c"))
    scale = 1.0 / math.sqrt(D)

    def at_x(d):
        return lax.rem(x + d + NX, NX)

    def at_y(d):
        return lax.rem(y + d + NY, NY)

    def at_z(d):
        return lax.rem(z + d + NZ, NZ)

    def copy(src, dst, send, recv, **where):
        return pltpu.make_async_remote_copy(
            src_ref=src, dst_ref=dst, send_sem=send, recv_sem=recv,
            device_id=where, device_id_type=MESH,
        )

    started = []

    def send(*args, **where):
        cp = copy(*args, **where)
        cp.start()
        started.append(cp)

    def arrived(ref, sem):
        copy(ref, ref, sem, sem, c=1 - c).wait_recv()

    barrier = pltpu.get_barrier_semaphore()
    peers = (
        [dict(x=at_x(d)) for d in range(1, NX)]
        + [dict(tok=at_y(d)) for d in range(1, NY)]
        + [dict(z=at_z(d)) for d in range(1, NZ)]
        + [dict(c=1 - c)]
    )
    for where in peers:
        pl.semaphore_signal(barrier, inc=1, device_id=where, device_id_type=MESH)

    fetch = pltpu.make_async_copy(signs_any, signs, signs_sem)
    fetch.start()
    table = inner_table()
    fetch.wait()
    signed = (table * signs[...]).astype(jnp.float32).astype(jnp.bfloat16)

    def piece(t, zz):
        return hb.at[t, :, pl.ds(pl.multiple_of(zz * 16, 16), 16), :]

    for t in range(NT3):
        for j in range(NX):
            first = j * TG + t * TT
            h = lax.dot_general(
                signed, picked[first : first + TT, :], NT, preferred_element_type=jnp.float32
            )
            hb[t, j] = h.astype(jnp.bfloat16)

    def scatter(t):
        for d in HOPS:
            send(piece(t, at_z(d)), x1.at[t, z], s2.at[t, d - 1], r2.at[t, d - 1], z=at_z(d))
        x1[t, z] = hb[t, :, pl.ds(pl.multiple_of(z * 16, 16), 16), :]

    def take(t, hops):
        for d in hops:
            arrived(x1.at[t, at_z(-d)], r2.at[t, d - 1])

    pl.semaphore_wait(barrier, len(peers))

    def scatter_x():
        for d in (2, 1, 3):
            send(hb.at[0, at_x(d)], xf.at[x], s1.at[0, d - 1], r1.at[0, d - 1], x=at_x(d))
        xf[x] = hb[0, x]

    def part_z(zz):
        return xf.at[:, pl.ds(pl.multiple_of(zz * 16, 16), 16), :]

    def scatter_z():
        for d in range(1, NX):
            arrived(xf.at[at_x(-d)], r1.at[0, d - 1])
        mine = x2.at[0, c, :, z]
        for d in HOPS:
            send(part_z(at_z(d)), mine, s2.at[0, d - 1], r2.at[0, d - 1], z=at_z(d))
        send(part_z(z), mine, s3.at[0, 0], r3.at[0, 0], c=1 - c)
        x2[0, c, :, z] = xf[:, pl.ds(pl.multiple_of(z * 16, 16), 16), :]

    def share_z():
        for d in HOPS:
            got = x2.at[0, c, :, at_z(-d)]
            arrived(got, r2.at[0, d - 1])
            send(got, got, s3.at[0, d], r3.at[0, d], c=1 - c)

    def exchange(t):
        for d in (2, 1, 3):
            send(
                x1.at[t, :, at_x(d)], x2.at[t, c, x], s1.at[t, d - 1], r1.at[t, d - 1], x=at_x(d)
            )
        send(x1.at[t, :, x], x2.at[t, c, x], s3.at[t, 0], r3.at[t, 0], c=1 - c)
        x2[t, c, x] = x1[t, :, x]

    def share_turned(t):
        for d in (1, 3, 2):
            got = x2.at[t, c, at_x(-d)]
            arrived(got, r1.at[t, d - 1])
            send(got, got, s3.at[t, d], r3.at[t, d], c=1 - c)

    def turn(t):
        for d in range(NX if t else NZ):
            theirs = x2.at[t, 1 - c, at_x(-d)] if t else x2.at[t, 1 - c, :, at_z(-d)]
            arrived(theirs, r3.at[t, d])
        spread = x2[t].reshape(1024, TT)

        def times(table):
            return (
                lax.dot_general(table[...], spread, NN, preferred_element_type=jnp.float32) * scale
            ).astype(jnp.bfloat16)

        rn[t] = times(hn).reshape(NZ, 64, TT)
        for d in HOPS:
            send(
                rn.at[t, at_z(d)], nz.at[z, y, t], sn.at[t, d - 1], rn_sem.at[t, d - 1], z=at_z(d)
            )
        nz[z, y, t] = rn[t, z]
        rows = times(hm)
        rm[t] = rows.reshape(NY, 128, TT)
        for d in range(1, NY):
            send(
                rm.at[t, at_y(d)], mb.at[z, c, y, t], sm.at[t, d - 1], rm_sem.at[t, d - 1],
                tok=at_y(d),
            )
        mb[z, c, y, t] = rm[t, y]
        sq = rows.astype(jnp.float32)
        return jnp.sum((sq * sq).reshape(64, 8, TT), axis=0)

    def near(t, d):
        got = nz.at[at_z(-d), y, t]
        send(got, got, sy.at[t, d, 0], ry.at[t, d, 0], tok=at_y(1))
        send(got, got, sy.at[t, d, 1], ry.at[t, d, 1], tok=at_y(-1))

    def far(t, d):
        left, right = nz.at[at_z(-d), at_y(-1), t], nz.at[at_z(-d), at_y(1), t]
        arrived(left, ry.at[t, d, 0])
        arrived(right, ry.at[t, d, 1])
        if (t + d) % 2 == 0:
            send(left, left, sy.at[t, d, 2], ry.at[t, d, 2], tok=at_y(1))
        else:
            send(right, right, sy.at[t, d, 2], ry.at[t, d, 2], tok=at_y(-1))

    stages = [
        [dict(c=1 - c)],
        [dict(x=at_x(d)) for d in range(1, NX)],
        [dict(tok=at_y(d)) for d in range(1, NY)],
        [dict(z=at_z(d)) for d in range(1, NZ)],
    ]
    base = [0, 1, 4, 7]

    def trace_send(k):
        for i, where in enumerate(stages[k]):
            j = base[k] + i
            send(ts.at[k], trx.at[j], st.at[j], rt.at[j], **where)

    def trace_take(k):
        total = ts[k]
        for i in range(len(stages[k])):
            j = base[k] + i
            arrived(trx.at[j], rt.at[j])
            total = total + trx[j]
        return total

    def ring(back, ahead, s, e):
        f = at_y(-e)
        if s < 4 or e < 2:
            got = mb.at[back, c, f]
            send(got, got, sr.at[s - 1, e], rr.at[s - 1, e], z=at_z(1))
        if s < 4 or e >= 2:
            got = mb.at[ahead, c, f]
            send(got, got, sl.at[s - 1, e], rl.at[s - 1, e], z=at_z(-1))

    def share(slot, k, e):
        got = mb.at[slot, c, at_y(-e)]
        send(got, got, sd.at[k, e], rd.at[k, e], c=1 - c)

    def ring_take(s, e):
        back, ahead, f = at_z(-s), at_z(s), at_y(-e)
        if s < 4 or e < 2:
            arrived(mb.at[back, c, f], rr.at[s - 1, e])
        if s < 4 or e >= 2:
            arrived(mb.at[ahead, c, f], rl.at[s - 1, e])
        if s < 4:
            ring(back, ahead, s + 1, e)
            share(back, 2 * s - 1, e)
            share(ahead, 2 * s, e)
        else:
            share(back, 7, e)

    scatter_x()
    scatter(1)
    scatter(2)
    hn[...] = outer_table(c, False)
    hm[...] = outer_table(c, True)
    scatter_z()
    take(1, HOPS)
    exchange(1)
    take(2, HOPS)
    exchange(2)
    share_turned(1)
    sq = turn(1)
    near(1, 0)
    share_z()
    share_turned(2)
    sq = sq + turn(2)
    near(2, 0)
    sq = sq + turn(0)
    near(0, 0)
    ts[0] = sq
    trace_send(0)
    for e in range(NY):
        if e:
            for t in range(NT3):
                arrived(mb.at[z, c, at_y(-e), t], rm_sem.at[t, e - 1])
        ring(z, z, 1, e)
        share(z, 0, e)
    def land(t):
        for d in HOPS:
            arrived(nz.at[at_z(-d), y, t], rn_sem.at[t, d - 1])
            near(t, d)

    def relay_own():
        for t in TILES:
            far(t, 0)

    def relay(t):
        for d in HOPS:
            far(t, d)

    land(1)
    relay_own()
    land(2)
    relay(1)
    land(0)
    ring_take(1, 0)
    relay(2)
    ring_take(1, 1)
    relay(0)
    ring_take(1, 2)
    ring_take(1, 3)
    ts[1] = trace_take(0)
    trace_send(1)

    order = column_order()
    for t in TILES:
        for d in range(NZ):
            arrived(nz.at[at_z(-d), at_y(2), t], ry.at[t, d, 2])
        for e in range(NY):
            lane = e * TG + t * TT
            for j in range(NX):
                part = nz[:, e, t, j * 16 : (j + 1) * 16, :].reshape(128, TT)
                np_[j * 128 : (j + 1) * 128, lane : lane + TT] = lax.dot_general(
                    order, part, NN, preferred_element_type=jnp.float32
                ).astype(jnp.bfloat16)

    slots = [z, at_z(-1), at_z(1), at_z(-2), at_z(2), at_z(-3), at_z(3), at_z(4)]
    right, left = at_x(1), at_x(-1)

    def multiply(k):
        slot = slots[k]
        for e in range(NY):
            arrived(mb.at[slot, 1 - c, at_y(-e)], rd.at[k, e])
        lhs = jnp.concatenate(
            [
                jnp.concatenate(
                    [mb[slot, e, f, t] for f in range(NY) for t in range(NT3)], axis=1
                )
                for e in range(NC)
            ],
            axis=0,
        )
        prod = lax.dot_general(lhs, np_[...], NT, preferred_element_type=jnp.float32)
        for j in range(NX):
            g[k, j] = prod[:, j * 128 : (j + 1) * 128]
        apart = g.at[k, at_x(2)]
        send(apart.at[0:128], ra.at[k, 0], sa.at[k, 0], ra_sem.at[k, 0], x=right)
        send(apart.at[128:256], ra.at[k, 1], sa.at[k, 1], ra_sem.at[k, 1], x=left)
        hand(k, 0, 1)
        hand(k, 1, 0)

    def hand(k, side, half):
        to = (right, left)[side]
        src = g.at[k, to, half * 128 : half * 128 + 128]
        send(
            src, rb.at[k, side, half], sb.at[k, side, half], rb_sem.at[k, side, half], x=to
        )

    def pass_on(k):
        for side, to in ((0, right), (1, left)):
            arrived(ra.at[k, side], ra_sem.at[k, side])
            rows = slice(side * 128, side * 128 + 128)
            g[k, to, rows, :] = g[k, to, rows, :] + ra[k, side]
            hand(k, side, side)

    def finish(k):
        for half in (1, 0):
            arrived(rb.at[k, half, 1 - half], rb_sem.at[k, half, 1 - half])
        for half in range(2):
            arrived(rb.at[k, half, half], rb_sem.at[k, half, half])
        for half in range(2):
            rows = slice(half * 128, half * 128 + 128)
            total = g[k, x, rows, :] + rb[k, 0, half] + rb[k, 1, half]
            for i in range(16):
                start = half * 128 + (i >> 2) * 32 + (i & 3) + slots[k] * 4
                out[pl.ds(start, 8, stride=256), :] = total[i * 8 : (i + 1) * 8, :]

    multiply(0)
    multiply(1)
    multiply(2)
    ring_take(2, 0)
    pass_on(0)
    ring_take(2, 1)
    pass_on(1)
    ring_take(2, 2)
    ring_take(2, 3)
    multiply(3)
    multiply(4)
    ring_take(3, 0)
    finish(0)
    pass_on(2)
    ring_take(3, 1)
    finish(1)
    ring_take(3, 2)
    pass_on(3)
    ring_take(3, 3)
    multiply(5)
    finish(2)
    multiply(6)
    ring_take(4, 0)
    pass_on(4)
    ring_take(4, 1)
    finish(3)
    ring_take(4, 2)
    pass_on(5)
    ring_take(4, 3)
    multiply(7)
    ts[2] = trace_take(1)
    trace_send(2)
    finish(4)
    pass_on(6)
    ts[3] = trace_take(2)
    trace_send(3)
    finish(5)
    pass_on(7)
    trace = jnp.sum(trace_take(3))
    finish(6)
    finish(7)

    i = lax.broadcasted_iota(jnp.int32, (128, 128), 0)
    j = lax.broadcasted_iota(jnp.int32, (128, 128), 1)
    block = pl.ds(pl.multiple_of(((z & 1) * 8 + x * 2 + c) * 128, 128), 128)
    on_diag = jnp.where((i == j) & (y == (z >> 1)), damping[0] * (trace / D), 0.0)
    out[block, :] = out[block, :] + on_diag
    for cp in started:
        cp.wait_send()


def rotate_and_multiply(damping, picked, signs):
    bf, f32 = jnp.bfloat16, jnp.float32
    V = pltpu.VMEM
    dma = pltpu.SemaphoreType.DMA
    scratch = [
        V((1, 128), jnp.int32),
        dma(()),
        V((NX, 128, TT), bf),
        V((NT3, NX, 128, TT), bf),
        V((NT3, NZ, NX, 16, TT), bf),
        V((NT3, NC, NX, NZ, 16, TT), bf),
        V((512, 1024), bf),
        V((512, 1024), bf),
        V((NT3, NY, 128, TT), bf),
        V((NT3, NZ, 64, TT), bf),
        V((NZ, NC, NY, NT3, 128, TT), bf),
        V((NZ, NY, NT3, 64, TT), bf),
        V((512, NY * TG), bf),
        V((NZ, NX, 256, 128), f32),
        V((NZ, 2, 128, 128), f32),
        V((NZ, 2, 2, 128, 128), f32),
        V((4, 8, 128), f32),
        V((14, 8, 128), f32),
    ] + [
        dma(shape)
        for shape in (
            (NT3, 3), (NT3, 7), (NT3, 8), (NT3, 7), (NT3, 3), (NT3, 8, 3),
            (4, 4), (4, 4), (8, 4), (8, 2), (8, 2, 2), (14,),
        )
        for _ in range(2)
    ]
    vmem = pl.BlockSpec(memory_space=pltpu.VMEM)
    smem = pl.BlockSpec(memory_space=pltpu.SMEM)
    hbm = pl.BlockSpec(memory_space=pltpu.MemorySpace.HBM)
    return pl.pallas_call(
        kernel,
        out_shape=jax.ShapeDtypeStruct((2048, 128), f32),
        in_specs=[smem, vmem, hbm],
        out_specs=vmem,
        scratch_shapes=scratch,
        compiler_params=pltpu.CompilerParams(
            collective_id=0, has_side_effects=True, vmem_limit_bytes=48 * 1024 * 1024
        ),
    )(damping, picked, signs)


def shards(row_bank, token_ids, sign_flips, damping):
    picked = lax.gather(
        row_bank,
        token_ids[:, None],
        lax.GatherDimensionNumbers((1,), (0,), (0,)),
        (1, row_bank.shape[1]),
        mode=lax.GatherScatterMode.PROMISE_IN_BOUNDS,
    )
    return rotate_and_multiply(damping, picked, sign_flips[None, :]) / TOKENS


def solution(mesh):
    split = Mesh(mesh.devices.reshape(NY, NZ, NX, NC), ("tok",) + COL)
    return jax.shard_map(
        shards,
        mesh=split,
        in_specs=(P(None, COL), P("tok"), P(COL), P()),
        out_specs=P("tok", COL),
        check_vma=False,
    )
```

```python
import math

import jax
import jax.numpy as jnp
from jax import lax
from jax.experimental import pallas as pl
from jax.experimental.pallas import tpu as pltpu
from jax.sharding import Mesh
from jax.sharding import PartitionSpec as P

D = 8192
BLOCK = 32
TOKENS = 6144
COL = ("z", "x", "c")
NY, NZ, NX, NC = 4, 8, 4, 2
TG = TOKENS // (NY * NX)
TT = 128
NT3 = TG // TT
HOPS = (4, 3, 5, 2, 6, 1, 7)
TILES = (1, 2, 0)
MESH = pl.DeviceIdType.MESH
NT = (((1,), (1,)), ((), ()))
NN = (((1,), (0,)), ((), ()))


def parity_sign(v):
    v = v ^ (v >> 4)
    v = v ^ (v >> 2)
    v = v ^ (v >> 1)
    return 1 - 2 * (v & 1)


def inner_table():
    r = lax.broadcasted_iota(jnp.int32, (128, 128), 0)
    k = lax.broadcasted_iota(jnp.int32, (128, 128), 1)
    b_r = ((r >> 4) << 2) | (r & 3)
    sign = parity_sign(b_r & (k & 31))
    return jnp.where(((r >> 2) & 3) == (k >> 5), sign, 0)


def outer_table(core, for_rows):
    k = lax.broadcasted_iota(jnp.int32, (1, 1024), 1)
    a = (((k >> 4) & 7) << 5) | (((k >> 7) & 3) << 3) | ((k >> 9) << 2) | ((k >> 2) & 3)

    def bits(r):
        if for_rows:
            return ((r >> 7) << 6) | ((r & 7) << 3) | ((r >> 5) & 3), (r >> 3) & 3
        return ((r >> 6) << 5) | (((r >> 4) & 3) << 3) | ((r >> 2) & 3), r & 3

    c_group, b_group = bits(lax.broadcasted_iota(jnp.int32, (64, 1), 0) * 8)
    c_place, b_place = bits(lax.broadcasted_iota(jnp.int32, (8, 1), 0))
    group = parity_sign((c_group | (core << 2)) & a)
    place = parity_sign(c_place & a)
    if for_rows:
        group = jnp.where(b_group == (k & 3), group, 0)
    else:
        place = jnp.where(b_place == (k & 3), place, 0)
    group, place = group.astype(jnp.float32), place.astype(jnp.float32)
    table = group[:, None, :] * place[None, :, :]
    return table.reshape(512, 1024).astype(jnp.bfloat16)


def column_order():
    o = lax.broadcasted_iota(jnp.int32, (128, 128), 0)
    i = lax.broadcasted_iota(jnp.int32, (128, 128), 1)
    src = (((o >> 2) & 7) << 4) | ((o >> 5) << 2) | (o & 3)
    return (i == src).astype(jnp.float32).astype(jnp.bfloat16)


def kernel(
    damping, picked, signs_any, out,
    signs, signs_sem, xf, hb, x1, x2, hm, hn, rm, rn, mb, nz, np_, g, ra, rb, ts, trx,
    s1, r1, s2, r2, s3, r3, sn, rn_sem, sm, rm_sem, sy, ry, sr, rr, sl, rl, sd, rd,
    sa, ra_sem, sb, rb_sem, st, rt,
):
    y, z, x, c = (lax.axis_index(n) for n in ("tok", "z", "x", "c"))
    scale = 1.0 / math.sqrt(D)

    def at_x(d):
        return lax.rem(x + d + NX, NX)

    def at_y(d):
        return lax.rem(y + d + NY, NY)

    def at_z(d):
        return lax.rem(z + d + NZ, NZ)

    def copy(src, dst, send, recv, **where):
        return pltpu.make_async_remote_copy(
            src_ref=src, dst_ref=dst, send_sem=send, recv_sem=recv,
            device_id=where, device_id_type=MESH,
        )

    started = []

    def send(*args, **where):
        cp = copy(*args, **where)
        cp.start()
        started.append(cp)

    def arrived(ref, sem):
        copy(ref, ref, sem, sem, c=1 - c).wait_recv()

    barrier = pltpu.get_barrier_semaphore()
    peers = (
        [dict(x=at_x(d)) for d in range(1, NX)]
        + [dict(tok=at_y(d)) for d in range(1, NY)]
        + [dict(z=at_z(d)) for d in range(1, NZ)]
        + [dict(c=1 - c)]
    )
    for where in peers:
        pl.semaphore_signal(barrier, inc=1, device_id=where, device_id_type=MESH)

    fetch = pltpu.make_async_copy(signs_any, signs, signs_sem)
    fetch.start()
    table = inner_table()
    fetch.wait()
    signed = (table * signs[...]).astype(jnp.float32).astype(jnp.bfloat16)

    def piece(t, zz):
        return hb.at[t, :, pl.ds(pl.multiple_of(zz * 16, 16), 16), :]

    for t in range(NT3):
        for j in range(NX):
            first = j * TG + t * TT
            h = lax.dot_general(
                signed, picked[first : first + TT, :], NT, preferred_element_type=jnp.float32
            )
            hb[t, j] = h.astype(jnp.bfloat16)

    def scatter(t):
        for d in HOPS:
            send(piece(t, at_z(d)), x1.at[t, z], s2.at[t, d - 1], r2.at[t, d - 1], z=at_z(d))
        x1[t, z] = hb[t, :, pl.ds(pl.multiple_of(z * 16, 16), 16), :]

    def take(t, hops):
        for d in hops:
            arrived(x1.at[t, at_z(-d)], r2.at[t, d - 1])

    pl.semaphore_wait(barrier, len(peers))

    def scatter_x():
        for d in (2, 1, 3):
            send(hb.at[0, at_x(d)], xf.at[x], s1.at[0, d - 1], r1.at[0, d - 1], x=at_x(d))
        xf[x] = hb[0, x]

    def part_z(zz):
        return xf.at[:, pl.ds(pl.multiple_of(zz * 16, 16), 16), :]

    def scatter_z():
        for d in range(1, NX):
            arrived(xf.at[at_x(-d)], r1.at[0, d - 1])
        mine = x2.at[0, c, :, z]
        for d in HOPS:
            send(part_z(at_z(d)), mine, s2.at[0, d - 1], r2.at[0, d - 1], z=at_z(d))
        send(part_z(z), mine, s3.at[0, 0], r3.at[0, 0], c=1 - c)
        x2[0, c, :, z] = xf[:, pl.ds(pl.multiple_of(z * 16, 16), 16), :]

    def share_z():
        for d in HOPS:
            got = x2.at[0, c, :, at_z(-d)]
            arrived(got, r2.at[0, d - 1])
            send(got, got, s3.at[0, d], r3.at[0, d], c=1 - c)

    def exchange(t):
        for d in (2, 1, 3):
            send(
                x1.at[t, :, at_x(d)], x2.at[t, c, x], s1.at[t, d - 1], r1.at[t, d - 1], x=at_x(d)
            )
        send(x1.at[t, :, x], x2.at[t, c, x], s3.at[t, 0], r3.at[t, 0], c=1 - c)
        x2[t, c, x] = x1[t, :, x]

    def share_turned(t):
        for d in (1, 3, 2):
            got = x2.at[t, c, at_x(-d)]
            arrived(got, r1.at[t, d - 1])
            send(got, got, s3.at[t, d], r3.at[t, d], c=1 - c)

    def turn(t):
        for d in range(NX if t else NZ):
            theirs = x2.at[t, 1 - c, at_x(-d)] if t else x2.at[t, 1 - c, :, at_z(-d)]
            arrived(theirs, r3.at[t, d])
        spread = x2[t].reshape(1024, TT)

        def times(table):
            return (
                lax.dot_general(table[...], spread, NN, preferred_element_type=jnp.float32) * scale
            ).astype(jnp.bfloat16)

        rn[t] = times(hn).reshape(NZ, 64, TT)
        for d in HOPS:
            send(
                rn.at[t, at_z(d)], nz.at[z, y, t], sn.at[t, d - 1], rn_sem.at[t, d - 1], z=at_z(d)
            )
        nz[z, y, t] = rn[t, z]
        rows = times(hm)
        rm[t] = rows.reshape(NY, 128, TT)
        for d in range(1, NY):
            send(
                rm.at[t, at_y(d)], mb.at[z, c, y, t], sm.at[t, d - 1], rm_sem.at[t, d - 1],
                tok=at_y(d),
            )
        mb[z, c, y, t] = rm[t, y]
        sq = rows.astype(jnp.float32)
        return jnp.sum((sq * sq).reshape(64, 8, TT), axis=0)

    def near(t, d):
        got = nz.at[at_z(-d), y, t]
        send(got, got, sy.at[t, d, 0], ry.at[t, d, 0], tok=at_y(1))
        send(got, got, sy.at[t, d, 1], ry.at[t, d, 1], tok=at_y(-1))

    def far(t, d):
        left, right = nz.at[at_z(-d), at_y(-1), t], nz.at[at_z(-d), at_y(1), t]
        arrived(left, ry.at[t, d, 0])
        arrived(right, ry.at[t, d, 1])
        if (t + d) % 2 == 0:
            send(left, left, sy.at[t, d, 2], ry.at[t, d, 2], tok=at_y(1))
        else:
            send(right, right, sy.at[t, d, 2], ry.at[t, d, 2], tok=at_y(-1))

    stages = [
        [dict(c=1 - c)],
        [dict(x=at_x(d)) for d in range(1, NX)],
        [dict(tok=at_y(d)) for d in range(1, NY)],
        [dict(z=at_z(d)) for d in range(1, NZ)],
    ]
    base = [0, 1, 4, 7]

    def trace_send(k):
        for i, where in enumerate(stages[k]):
            j = base[k] + i
            send(ts.at[k], trx.at[j], st.at[j], rt.at[j], **where)

    def trace_take(k):
        total = ts[k]
        for i in range(len(stages[k])):
            j = base[k] + i
            arrived(trx.at[j], rt.at[j])
            total = total + trx[j]
        return total

    def ring(back, ahead, s, e):
        f = at_y(-e)
        if s < 4 or e < 2:
            got = mb.at[back, c, f]
            send(got, got, sr.at[s - 1, e], rr.at[s - 1, e], z=at_z(1))
        if s < 4 or e >= 2:
            got = mb.at[ahead, c, f]
            send(got, got, sl.at[s - 1, e], rl.at[s - 1, e], z=at_z(-1))

    def share(slot, k, e):
        got = mb.at[slot, c, at_y(-e)]
        send(got, got, sd.at[k, e], rd.at[k, e], c=1 - c)

    def ring_take(s, e):
        back, ahead, f = at_z(-s), at_z(s), at_y(-e)
        if s < 4 or e < 2:
            arrived(mb.at[back, c, f], rr.at[s - 1, e])
        if s < 4 or e >= 2:
            arrived(mb.at[ahead, c, f], rl.at[s - 1, e])
        if s < 4:
            ring(back, ahead, s + 1, e)
            share(back, 2 * s - 1, e)
            share(ahead, 2 * s, e)
        else:
            share(back, 7, e)

    scatter_x()
    scatter(1)
    scatter(2)
    scatter_z()
    hn[...] = outer_table(c, False)
    hm[...] = outer_table(c, True)
    take(1, HOPS)
    exchange(1)
    take(2, HOPS)
    exchange(2)
    share_turned(1)
    sq = turn(1)
    near(1, 0)
    share_z()
    share_turned(2)
    sq = sq + turn(2)
    near(2, 0)
    sq = sq + turn(0)
    near(0, 0)
    ts[0] = sq
    trace_send(0)
    for e in range(NY):
        if e:
            for t in range(NT3):
                arrived(mb.at[z, c, at_y(-e), t], rm_sem.at[t, e - 1])
        ring(z, z, 1, e)
        share(z, 0, e)
    def land(t):
        for d in HOPS:
            arrived(nz.at[at_z(-d), y, t], rn_sem.at[t, d - 1])
            near(t, d)

    def relay_own():
        for t in TILES:
            far(t, 0)

    def relay(t):
        for d in HOPS:
            far(t, d)

    land(1)
    relay_own()
    land(2)
    relay(1)
    land(0)
    ring_take(1, 0)
    relay(2)
    ring_take(1, 1)
    relay(0)
    ring_take(1, 2)
    ring_take(1, 3)
    ts[1] = trace_take(0)
    trace_send(1)

    order = column_order()
    for t in TILES:
        for d in range(NZ):
            arrived(nz.at[at_z(-d), at_y(2), t], ry.at[t, d, 2])
        for e in range(NY):
            lane = e * TG + t * TT
            for j in range(NX):
                part = nz[:, e, t, j * 16 : (j + 1) * 16, :].reshape(128, TT)
                np_[j * 128 : (j + 1) * 128, lane : lane + TT] = lax.dot_general(
                    order, part, NN, preferred_element_type=jnp.float32
                ).astype(jnp.bfloat16)

    slots = [z, at_z(-1), at_z(1), at_z(-2), at_z(2), at_z(-3), at_z(3), at_z(4)]
    right, left = at_x(1), at_x(-1)

    def multiply(k):
        slot = slots[k]
        for e in range(NY):
            arrived(mb.at[slot, 1 - c, at_y(-e)], rd.at[k, e])
        lhs = jnp.concatenate(
            [
                jnp.concatenate(
                    [mb[slot, e, f, t] for f in range(NY) for t in range(NT3)], axis=1
                )
                for e in range(NC)
            ],
            axis=0,
        )
        prod = lax.dot_general(lhs, np_[...], NT, preferred_element_type=jnp.float32)
        for j in range(NX):
            g[k, j] = prod[:, j * 128 : (j + 1) * 128]
        apart = g.at[k, at_x(2)]
        send(apart.at[0:128], ra.at[k, 0], sa.at[k, 0], ra_sem.at[k, 0], x=right)
        send(apart.at[128:256], ra.at[k, 1], sa.at[k, 1], ra_sem.at[k, 1], x=left)
        hand(k, 0, 1)
        hand(k, 1, 0)

    def hand(k, side, half):
        to = (right, left)[side]
        src = g.at[k, to, half * 128 : half * 128 + 128]
        send(
            src, rb.at[k, side, half], sb.at[k, side, half], rb_sem.at[k, side, half], x=to
        )

    def pass_on(k):
        for side, to in ((0, right), (1, left)):
            arrived(ra.at[k, side], ra_sem.at[k, side])
            rows = slice(side * 128, side * 128 + 128)
            g[k, to, rows, :] = g[k, to, rows, :] + ra[k, side]
            hand(k, side, side)

    def finish(k):
        for half in (1, 0):
            arrived(rb.at[k, half, 1 - half], rb_sem.at[k, half, 1 - half])
        for half in range(2):
            arrived(rb.at[k, half, half], rb_sem.at[k, half, half])
        for half in range(2):
            rows = slice(half * 128, half * 128 + 128)
            total = g[k, x, rows, :] + rb[k, 0, half] + rb[k, 1, half]
            for i in range(16):
                start = half * 128 + (i >> 2) * 32 + (i & 3) + slots[k] * 4
                out[pl.ds(start, 8, stride=256), :] = total[i * 8 : (i + 1) * 8, :]

    multiply(0)
    multiply(1)
    multiply(2)
    ring_take(2, 0)
    ring_take(2, 1)
    ring_take(2, 2)
    pass_on(0)
    ring_take(2, 3)
    multiply(3)
    multiply(4)
    pass_on(1)
    ring_take(3, 0)
    ring_take(3, 1)
    finish(0)
    pass_on(2)
    ring_take(3, 2)
    ring_take(3, 3)
    multiply(5)
    multiply(6)
    pass_on(3)
    finish(1)
    ring_take(4, 0)
    ring_take(4, 1)
    pass_on(4)
    finish(2)
    ring_take(4, 2)
    ring_take(4, 3)
    multiply(7)
    ts[2] = trace_take(1)
    trace_send(2)
    pass_on(5)
    finish(3)
    pass_on(6)
    finish(4)
    ts[3] = trace_take(2)
    trace_send(3)
    pass_on(7)
    finish(5)
    trace = jnp.sum(trace_take(3))
    finish(6)
    finish(7)

    i = lax.broadcasted_iota(jnp.int32, (128, 128), 0)
    j = lax.broadcasted_iota(jnp.int32, (128, 128), 1)
    block = pl.ds(pl.multiple_of(((z & 1) * 8 + x * 2 + c) * 128, 128), 128)
    on_diag = jnp.where((i == j) & (y == (z >> 1)), damping[0] * (trace / D), 0.0)
    out[block, :] = out[block, :] + on_diag
    for cp in started:
        cp.wait_send()


def rotate_and_multiply(damping, picked, signs):
    bf, f32 = jnp.bfloat16, jnp.float32
    V = pltpu.VMEM
    dma = pltpu.SemaphoreType.DMA
    scratch = [
        V((1, 128), jnp.int32),
        dma(()),
        V((NX, 128, TT), bf),
        V((NT3, NX, 128, TT), bf),
        V((NT3, NZ, NX, 16, TT), bf),
        V((NT3, NC, NX, NZ, 16, TT), bf),
        V((512, 1024), bf),
        V((512, 1024), bf),
        V((NT3, NY, 128, TT), bf),
        V((NT3, NZ, 64, TT), bf),
        V((NZ, NC, NY, NT3, 128, TT), bf),
        V((NZ, NY, NT3, 64, TT), bf),
        V((512, NY * TG), bf),
        V((NZ, NX, 256, 128), f32),
        V((NZ, 2, 128, 128), f32),
        V((NZ, 2, 2, 128, 128), f32),
        V((4, 8, 128), f32),
        V((14, 8, 128), f32),
    ] + [
        dma(shape)
        for shape in (
            (NT3, 3), (NT3, 7), (NT3, 8), (NT3, 7), (NT3, 3), (NT3, 8, 3),
            (4, 4), (4, 4), (8, 4), (8, 2), (8, 2, 2), (14,),
        )
        for _ in range(2)
    ]
    vmem = pl.BlockSpec(memory_space=pltpu.VMEM)
    smem = pl.BlockSpec(memory_space=pltpu.SMEM)
    hbm = pl.BlockSpec(memory_space=pltpu.MemorySpace.HBM)
    return pl.pallas_call(
        kernel,
        out_shape=jax.ShapeDtypeStruct((2048, 128), f32),
        in_specs=[smem, vmem, hbm],
        out_specs=vmem,
        scratch_shapes=scratch,
        compiler_params=pltpu.CompilerParams(
            collective_id=0, has_side_effects=True, vmem_limit_bytes=48 * 1024 * 1024
        ),
    )(damping, picked, signs)


def shards(row_bank, token_ids, sign_flips, damping):
    picked = lax.gather(
        row_bank,
        token_ids[:, None],
        lax.GatherDimensionNumbers((1,), (0,), (0,)),
        (1, row_bank.shape[1]),
        mode=lax.GatherScatterMode.PROMISE_IN_BOUNDS,
    )
    return rotate_and_multiply(damping, picked, sign_flips[None, :]) / TOKENS


def solution(mesh):
    split = Mesh(mesh.devices.reshape(NY, NZ, NX, NC), ("tok",) + COL)
    return jax.shard_map(
        shards,
        mesh=split,
        in_specs=(P(None, COL), P("tok"), P(COL), P()),
        out_specs=P("tok", COL),
        check_vma=False,
    )
```

```python
import math

import jax
import jax.numpy as jnp
from jax import lax
from jax.experimental import pallas as pl
from jax.experimental.pallas import tpu as pltpu
from jax.sharding import Mesh
from jax.sharding import PartitionSpec as P

D = 8192
BLOCK = 32
TOKENS = 6144
COL = ("z", "x", "c")
NY, NZ, NX, NC = 4, 8, 4, 2
TG = TOKENS // (NY * NX)
TT = 128
NT3 = TG // TT
HOPS = (4, 3, 5, 2, 6, 1, 7)
TILES = (1, 2, 0)
MESH = pl.DeviceIdType.MESH
NT = (((1,), (1,)), ((), ()))
NN = (((1,), (0,)), ((), ()))


def parity_sign(v):
    v = v ^ (v >> 4)
    v = v ^ (v >> 2)
    v = v ^ (v >> 1)
    return 1 - 2 * (v & 1)


def inner_table():
    r = lax.broadcasted_iota(jnp.int32, (128, 128), 0)
    k = lax.broadcasted_iota(jnp.int32, (128, 128), 1)
    b_r = ((r >> 4) << 2) | (r & 3)
    sign = parity_sign(b_r & (k & 31))
    return jnp.where(((r >> 2) & 3) == (k >> 5), sign, 0)


def outer_table(core, for_rows):
    k = lax.broadcasted_iota(jnp.int32, (1, 1024), 1)
    a = (((k >> 4) & 7) << 5) | (((k >> 7) & 3) << 3) | ((k >> 9) << 2) | ((k >> 2) & 3)

    def bits(r):
        if for_rows:
            return ((r >> 7) << 6) | ((r & 7) << 3) | ((r >> 5) & 3), (r >> 3) & 3
        return ((r >> 6) << 5) | (((r >> 4) & 3) << 3) | ((r >> 2) & 3), r & 3

    c_group, b_group = bits(lax.broadcasted_iota(jnp.int32, (64, 1), 0) * 8)
    c_place, b_place = bits(lax.broadcasted_iota(jnp.int32, (8, 1), 0))
    group = parity_sign((c_group | (core << 2)) & a)
    place = parity_sign(c_place & a)
    if for_rows:
        group = jnp.where(b_group == (k & 3), group, 0)
    else:
        place = jnp.where(b_place == (k & 3), place, 0)
    group, place = group.astype(jnp.float32), place.astype(jnp.float32)
    table = group[:, None, :] * place[None, :, :]
    return table.reshape(512, 1024).astype(jnp.bfloat16)


def column_order():
    o = lax.broadcasted_iota(jnp.int32, (128, 128), 0)
    i = lax.broadcasted_iota(jnp.int32, (128, 128), 1)
    src = (((o >> 2) & 7) << 4) | ((o >> 5) << 2) | (o & 3)
    return (i == src).astype(jnp.float32).astype(jnp.bfloat16)


def kernel(
    damping, picked, signs, out,
    xf, hb, x1, x2, hm, hn, rm, rn, mb, nz, np_, g, ra, rb, ts, trx,
    s1, r1, s2, r2, s3, r3, sn, rn_sem, sm, rm_sem, sy, ry, sr, rr, sl, rl, sd, rd,
    sa, ra_sem, sb, rb_sem, st, rt,
):
    y, z, x, c = (lax.axis_index(n) for n in ("tok", "z", "x", "c"))
    scale = 1.0 / math.sqrt(D)

    def at_x(d):
        return lax.rem(x + d + NX, NX)

    def at_y(d):
        return lax.rem(y + d + NY, NY)

    def at_z(d):
        return lax.rem(z + d + NZ, NZ)

    def copy(src, dst, send, recv, **where):
        return pltpu.make_async_remote_copy(
            src_ref=src, dst_ref=dst, send_sem=send, recv_sem=recv,
            device_id=where, device_id_type=MESH,
        )

    started = []

    def send(*args, **where):
        cp = copy(*args, **where)
        cp.start()
        started.append(cp)

    def arrived(ref, sem):
        copy(ref, ref, sem, sem, c=1 - c).wait_recv()

    barrier = pltpu.get_barrier_semaphore()
    peers = (
        [dict(x=at_x(d)) for d in range(1, NX)]
        + [dict(tok=at_y(d)) for d in range(1, NY)]
        + [dict(z=at_z(d)) for d in range(1, NZ)]
        + [dict(c=1 - c)]
    )
    for where in peers:
        pl.semaphore_signal(barrier, inc=1, device_id=where, device_id_type=MESH)

    table = inner_table()
    lane = lax.broadcasted_iota(jnp.int32, (1, 128), 1)
    row = jnp.zeros((1, 128), jnp.int32)
    for i in range(128):
        row = jnp.where(lane == i, signs[i], row)
    signed = (table * row).astype(jnp.float32).astype(jnp.bfloat16)

    def piece(t, zz):
        return hb.at[t, :, pl.ds(pl.multiple_of(zz * 16, 16), 16), :]

    for t in range(NT3):
        for j in range(NX):
            first = j * TG + t * TT
            h = lax.dot_general(
                signed, picked[first : first + TT, :], NT, preferred_element_type=jnp.float32
            )
            hb[t, j] = h.astype(jnp.bfloat16)

    def scatter(t):
        for d in HOPS:
            send(piece(t, at_z(d)), x1.at[t, z], s2.at[t, d - 1], r2.at[t, d - 1], z=at_z(d))
        x1[t, z] = hb[t, :, pl.ds(pl.multiple_of(z * 16, 16), 16), :]

    def take(t, hops):
        for d in hops:
            arrived(x1.at[t, at_z(-d)], r2.at[t, d - 1])

    pl.semaphore_wait(barrier, len(peers))

    def scatter_x():
        for d in (2, 1, 3):
            send(hb.at[0, at_x(d)], xf.at[x], s1.at[0, d - 1], r1.at[0, d - 1], x=at_x(d))
        xf[x] = hb[0, x]

    def part_z(zz):
        return xf.at[:, pl.ds(pl.multiple_of(zz * 16, 16), 16), :]

    def scatter_z():
        for d in range(1, NX):
            arrived(xf.at[at_x(-d)], r1.at[0, d - 1])
        mine = x2.at[0, c, :, z]
        for d in HOPS:
            send(part_z(at_z(d)), mine, s2.at[0, d - 1], r2.at[0, d - 1], z=at_z(d))
        send(part_z(z), mine, s3.at[0, 0], r3.at[0, 0], c=1 - c)
        x2[0, c, :, z] = xf[:, pl.ds(pl.multiple_of(z * 16, 16), 16), :]

    def share_z():
        for d in HOPS:
            got = x2.at[0, c, :, at_z(-d)]
            arrived(got, r2.at[0, d - 1])
            send(got, got, s3.at[0, d], r3.at[0, d], c=1 - c)

    def exchange(t):
        for d in (2, 1, 3):
            send(
                x1.at[t, :, at_x(d)], x2.at[t, c, x], s1.at[t, d - 1], r1.at[t, d - 1], x=at_x(d)
            )
        send(x1.at[t, :, x], x2.at[t, c, x], s3.at[t, 0], r3.at[t, 0], c=1 - c)
        x2[t, c, x] = x1[t, :, x]

    def share_turned(t):
        for d in (1, 3, 2):
            got = x2.at[t, c, at_x(-d)]
            arrived(got, r1.at[t, d - 1])
            send(got, got, s3.at[t, d], r3.at[t, d], c=1 - c)

    def turn(t):
        for d in range(NX if t else NZ):
            theirs = x2.at[t, 1 - c, at_x(-d)] if t else x2.at[t, 1 - c, :, at_z(-d)]
            arrived(theirs, r3.at[t, d])
        spread = x2[t].reshape(1024, TT)

        def times(table):
            return (
                lax.dot_general(table[...], spread, NN, preferred_element_type=jnp.float32) * scale
            ).astype(jnp.bfloat16)

        rn[t] = times(hn).reshape(NZ, 64, TT)
        for d in HOPS:
            send(
                rn.at[t, at_z(d)], nz.at[z, y, t], sn.at[t, d - 1], rn_sem.at[t, d - 1], z=at_z(d)
            )
        nz[z, y, t] = rn[t, z]
        rows = times(hm)
        rm[t] = rows.reshape(NY, 128, TT)
        for d in range(1, NY):
            send(
                rm.at[t, at_y(d)], mb.at[z, c, y, t], sm.at[t, d - 1], rm_sem.at[t, d - 1],
                tok=at_y(d),
            )
        mb[z, c, y, t] = rm[t, y]
        sq = rows.astype(jnp.float32)
        return jnp.sum((sq * sq).reshape(64, 8, TT), axis=0)

    def near(t, d):
        got = nz.at[at_z(-d), y, t]
        send(got, got, sy.at[t, d, 0], ry.at[t, d, 0], tok=at_y(1))
        send(got, got, sy.at[t, d, 1], ry.at[t, d, 1], tok=at_y(-1))

    def far(t, d):
        left, right = nz.at[at_z(-d), at_y(-1), t], nz.at[at_z(-d), at_y(1), t]
        arrived(left, ry.at[t, d, 0])
        arrived(right, ry.at[t, d, 1])
        if (t + d) % 2 == 0:
            send(left, left, sy.at[t, d, 2], ry.at[t, d, 2], tok=at_y(1))
        else:
            send(right, right, sy.at[t, d, 2], ry.at[t, d, 2], tok=at_y(-1))

    stages = [
        [dict(c=1 - c)],
        [dict(x=at_x(d)) for d in range(1, NX)],
        [dict(tok=at_y(d)) for d in range(1, NY)],
        [dict(z=at_z(d)) for d in range(1, NZ)],
    ]
    base = [0, 1, 4, 7]

    def trace_send(k):
        for i, where in enumerate(stages[k]):
            j = base[k] + i
            send(ts.at[k], trx.at[j], st.at[j], rt.at[j], **where)

    def trace_take(k):
        total = ts[k]
        for i in range(len(stages[k])):
            j = base[k] + i
            arrived(trx.at[j], rt.at[j])
            total = total + trx[j]
        return total

    def ring(back, ahead, s, e):
        f = at_y(-e)
        if s < 4 or e < 2:
            got = mb.at[back, c, f]
            send(got, got, sr.at[s - 1, e], rr.at[s - 1, e], z=at_z(1))
        if s < 4 or e >= 2:
            got = mb.at[ahead, c, f]
            send(got, got, sl.at[s - 1, e], rl.at[s - 1, e], z=at_z(-1))

    def share(slot, k, e):
        got = mb.at[slot, c, at_y(-e)]
        send(got, got, sd.at[k, e], rd.at[k, e], c=1 - c)

    def ring_take(s, e):
        back, ahead, f = at_z(-s), at_z(s), at_y(-e)
        if s < 4 or e < 2:
            arrived(mb.at[back, c, f], rr.at[s - 1, e])
        if s < 4 or e >= 2:
            arrived(mb.at[ahead, c, f], rl.at[s - 1, e])
        if s < 4:
            ring(back, ahead, s + 1, e)
            share(back, 2 * s - 1, e)
            share(ahead, 2 * s, e)
        else:
            share(back, 7, e)

    scatter_x()
    scatter(1)
    scatter(2)
    scatter_z()
    hn[...] = outer_table(c, False)
    hm[...] = outer_table(c, True)
    take(1, HOPS)
    exchange(1)
    take(2, HOPS)
    exchange(2)
    share_turned(1)
    sq = turn(1)
    near(1, 0)
    share_z()
    share_turned(2)
    sq = sq + turn(2)
    near(2, 0)
    sq = sq + turn(0)
    near(0, 0)
    ts[0] = sq
    trace_send(0)
    for e in range(NY):
        if e:
            for t in range(NT3):
                arrived(mb.at[z, c, at_y(-e), t], rm_sem.at[t, e - 1])
        ring(z, z, 1, e)
        share(z, 0, e)
    def land(t):
        for d in HOPS:
            arrived(nz.at[at_z(-d), y, t], rn_sem.at[t, d - 1])
            near(t, d)

    def relay_own():
        for t in TILES:
            far(t, 0)

    def relay(t):
        for d in HOPS:
            far(t, d)

    land(1)
    relay_own()
    land(2)
    relay(1)
    land(0)
    ring_take(1, 0)
    relay(2)
    ring_take(1, 1)
    relay(0)
    ring_take(1, 2)
    ring_take(1, 3)
    ts[1] = trace_take(0)
    trace_send(1)

    order = column_order()
    for t in TILES:
        for d in range(NZ):
            arrived(nz.at[at_z(-d), at_y(2), t], ry.at[t, d, 2])
        for e in range(NY):
            lane = e * TG + t * TT
            for j in range(NX):
                part = nz[:, e, t, j * 16 : (j + 1) * 16, :].reshape(128, TT)
                np_[j * 128 : (j + 1) * 128, lane : lane + TT] = lax.dot_general(
                    order, part, NN, preferred_element_type=jnp.float32
                ).astype(jnp.bfloat16)

    slots = [z, at_z(-1), at_z(1), at_z(-2), at_z(2), at_z(-3), at_z(3), at_z(4)]
    right, left = at_x(1), at_x(-1)

    def multiply(k):
        slot = slots[k]
        for e in range(NY):
            arrived(mb.at[slot, 1 - c, at_y(-e)], rd.at[k, e])
        lhs = jnp.concatenate(
            [
                jnp.concatenate(
                    [mb[slot, e, f, t] for f in range(NY) for t in range(NT3)], axis=1
                )
                for e in range(NC)
            ],
            axis=0,
        )
        prod = lax.dot_general(lhs, np_[...], NT, preferred_element_type=jnp.float32)
        for j in range(NX):
            g[k, j] = prod[:, j * 128 : (j + 1) * 128]
        apart = g.at[k, at_x(2)]
        send(apart.at[0:128], ra.at[k, 0], sa.at[k, 0], ra_sem.at[k, 0], x=right)
        send(apart.at[128:256], ra.at[k, 1], sa.at[k, 1], ra_sem.at[k, 1], x=left)
        hand(k, 0, 1)
        hand(k, 1, 0)

    def hand(k, side, half):
        to = (right, left)[side]
        src = g.at[k, to, half * 128 : half * 128 + 128]
        send(
            src, rb.at[k, side, half], sb.at[k, side, half], rb_sem.at[k, side, half], x=to
        )

    def pass_on(k):
        for side, to in ((0, right), (1, left)):
            arrived(ra.at[k, side], ra_sem.at[k, side])
            rows = slice(side * 128, side * 128 + 128)
            g[k, to, rows, :] = g[k, to, rows, :] + ra[k, side]
            hand(k, side, side)

    def finish(k):
        for half in (1, 0):
            arrived(rb.at[k, half, 1 - half], rb_sem.at[k, half, 1 - half])
        for half in range(2):
            arrived(rb.at[k, half, half], rb_sem.at[k, half, half])
        for half in range(2):
            rows = slice(half * 128, half * 128 + 128)
            total = g[k, x, rows, :] + rb[k, 0, half] + rb[k, 1, half]
            for i in range(16):
                start = half * 128 + (i >> 2) * 32 + (i & 3) + slots[k] * 4
                out[pl.ds(start, 8, stride=256), :] = total[i * 8 : (i + 1) * 8, :]

    multiply(0)
    multiply(1)
    multiply(2)
    ring_take(2, 0)
    ring_take(2, 1)
    ring_take(2, 2)
    pass_on(0)
    ring_take(2, 3)
    multiply(3)
    multiply(4)
    pass_on(1)
    ring_take(3, 0)
    ring_take(3, 1)
    finish(0)
    pass_on(2)
    ring_take(3, 2)
    ring_take(3, 3)
    multiply(5)
    multiply(6)
    pass_on(3)
    finish(1)
    ring_take(4, 0)
    ring_take(4, 1)
    pass_on(4)
    finish(2)
    ring_take(4, 2)
    ring_take(4, 3)
    multiply(7)
    ts[2] = trace_take(1)
    trace_send(2)
    pass_on(5)
    finish(3)
    pass_on(6)
    finish(4)
    ts[3] = trace_take(2)
    trace_send(3)
    pass_on(7)
    finish(5)
    trace = jnp.sum(trace_take(3))
    finish(6)
    finish(7)

    i = lax.broadcasted_iota(jnp.int32, (128, 128), 0)
    j = lax.broadcasted_iota(jnp.int32, (128, 128), 1)
    block = pl.ds(pl.multiple_of(((z & 1) * 8 + x * 2 + c) * 128, 128), 128)
    on_diag = jnp.where((i == j) & (y == (z >> 1)), damping[0] * (trace / D), 0.0)
    out[block, :] = out[block, :] + on_diag
    for cp in started:
        cp.wait_send()


def rotate_and_multiply(damping, picked, signs):
    bf, f32 = jnp.bfloat16, jnp.float32
    V = pltpu.VMEM
    dma = pltpu.SemaphoreType.DMA
    scratch = [
        V((NX, 128, TT), bf),
        V((NT3, NX, 128, TT), bf),
        V((NT3, NZ, NX, 16, TT), bf),
        V((NT3, NC, NX, NZ, 16, TT), bf),
        V((512, 1024), bf),
        V((512, 1024), bf),
        V((NT3, NY, 128, TT), bf),
        V((NT3, NZ, 64, TT), bf),
        V((NZ, NC, NY, NT3, 128, TT), bf),
        V((NZ, NY, NT3, 64, TT), bf),
        V((512, NY * TG), bf),
        V((NZ, NX, 256, 128), f32),
        V((NZ, 2, 128, 128), f32),
        V((NZ, 2, 2, 128, 128), f32),
        V((4, 8, 128), f32),
        V((14, 8, 128), f32),
    ] + [
        dma(shape)
        for shape in (
            (NT3, 3), (NT3, 7), (NT3, 8), (NT3, 7), (NT3, 3), (NT3, 8, 3),
            (4, 4), (4, 4), (8, 4), (8, 2), (8, 2, 2), (14,),
        )
        for _ in range(2)
    ]
    vmem = pl.BlockSpec(memory_space=pltpu.VMEM)
    smem = pl.BlockSpec(memory_space=pltpu.SMEM)
    return pl.pallas_call(
        kernel,
        out_shape=jax.ShapeDtypeStruct((2048, 128), f32),
        in_specs=[smem, vmem, smem],
        out_specs=vmem,
        scratch_shapes=scratch,
        compiler_params=pltpu.CompilerParams(
            collective_id=0, has_side_effects=True, vmem_limit_bytes=48 * 1024 * 1024
        ),
    )(damping, picked, signs)


def shards(row_bank, token_ids, sign_flips, damping):
    picked = lax.gather(
        row_bank,
        token_ids[:, None],
        lax.GatherDimensionNumbers((1,), (0,), (0,)),
        (1, row_bank.shape[1]),
        mode=lax.GatherScatterMode.PROMISE_IN_BOUNDS,
    )
    return rotate_and_multiply(damping, picked, sign_flips) / TOKENS


def solution(mesh):
    split = Mesh(mesh.devices.reshape(NY, NZ, NX, NC), ("tok",) + COL)
    return jax.shard_map(
        shards,
        mesh=split,
        in_specs=(P(None, COL), P("tok"), P(COL), P()),
        out_specs=P("tok", COL),
        check_vma=False,
    )
```
